32 devices in a mesh: dp: 2 (over x), tp: 4 (over z), cp: 4 (over y, core).
Axes of the slice: x: 2, y: 2, z: 4, core: 2. Of those that a mesh axis runs over, the one named last changes fastest.
Arguments:
- hidden: bfloat16 [8192, 3840], P(('dp', 'cp')), parts along dimension 0
- start_pos: int32 [2], P('dp'), parts along dimension 0
- k_local: bfloat16 [2048, 8, 256], P('dp', 'tp'), parts along dimension 0
- v_local: bfloat16 [2048, 8, 256], P('dp', 'tp'), parts along dimension 0
- k_global: bfloat16 [49152, 8, 256], P(('dp', 'cp'), 'tp'), parts along dimension 0
- v_global: bfloat16 [49152, 8, 256], P(('dp', 'cp'), 'tp'), parts along dimension 0
- w_query: bfloat16 [2, 3840, 4096], P(None, None, 'tp')
- w_key: bfloat16 [2, 3840, 2048], P(None, None, 'tp')
- w_value: bfloat16 [2, 3840, 2048], P(None, None, 'tp')
- w_out: bfloat16 [2, 4096, 3840], P(None, 'tp')
- w_gate: bfloat16 [2, 3840, 15360], P(None, None, 'tp')
- w_up: bfloat16 [2, 3840, 15360], P(None, None, 'tp')
- w_down: bfloat16 [2, 15360, 3840], P(None, 'tp')
- norm_gain: float32 [2, 4, 3840], replicated
- qk_gain: float32 [2, 2, 256], replicated
Outputs:
- output 1: bfloat16 [8192, 3840], P(('dp', 'cp')), parts along dimension 0
- output 2: bfloat16 [8192, 8, 256], P(('dp', 'cp'), 'tp'), parts along dimension 0
- output 3: bfloat16 [8192, 8, 256], P(('dp', 'cp'), 'tp'), parts along dimension 0
- output 4: bfloat16 [8192, 8, 256], P(('dp', 'cp'), 'tp'), parts along dimension 0
- output 5: bfloat16 [8192, 8, 256], P(('dp', 'cp'), 'tp'), parts along dimension 0
There are 2 independent parts. The reference program is written for one: setup_inputs(seed, part) draws one part's arguments, and reference() takes and returns one part's arrays. A program takes and returns all parts, laid end to end along the dimension named above; an argument that names none is the same for every part.
All inputs are finite; a program needn't handle non-finite values.
Results may differ from the reference program's by a relative error of at most 0.02.
Values are sent between devices in bfloat16 or wider.
A program may use at most 1 GiB of HBM per device.

```python
import jax
import jax.numpy as jnp
from jax import lax

MODEL_DIM = 3840
NUM_HEADS = 16
KV_HEADS = 8
HEAD_DIM = 256
FFN_DIM = 15360
WINDOW = 1024
CHUNK_LEN = 4096
CACHE_LEN = 24576
CACHE_SHARD = 6144
QUERY_BLOCK = 32

GROUPS = NUM_HEADS // KV_HEADS
NORM_EPS = 1e-6
LOCAL_BASE = 10000.0
GLOBAL_BASE = 1000000.0
GLOBAL_DIV = 8.0


def setup_inputs(seed: int = 0, part: int = 0) -> dict:
    part_key = jax.random.fold_in(jax.random.key(seed), part)
    own_keys = jax.random.split(part_key, 6)
    shared_keys = jax.random.split(jax.random.key(seed + 1), 9)

    def weight(draw_key, arr_shape, fan_in):
        return (jax.random.normal(draw_key, arr_shape, jnp.float32) * fan_in ** -0.5).astype(jnp.bfloat16)

    def unit_draw(draw_key, arr_shape):
        return jax.random.normal(draw_key, arr_shape, jnp.float32).astype(jnp.bfloat16)

    q_cols = NUM_HEADS * HEAD_DIM
    kv_cols = KV_HEADS * HEAD_DIM
    offset = jax.random.randint(own_keys[1], (1,), 0, CACHE_SHARD // 2 + 1)
    return {
        'hidden': unit_draw(own_keys[0], (CHUNK_LEN, MODEL_DIM)),
        'start_pos': (CACHE_LEN - offset).astype(jnp.int32),
        'k_local': unit_draw(own_keys[2], (WINDOW, KV_HEADS, HEAD_DIM)),
        'v_local': unit_draw(own_keys[3], (WINDOW, KV_HEADS, HEAD_DIM)),
        'k_global': unit_draw(own_keys[4], (CACHE_LEN, KV_HEADS, HEAD_DIM)),
        'v_global': unit_draw(own_keys[5], (CACHE_LEN, KV_HEADS, HEAD_DIM)),
        'w_query': weight(shared_keys[0], (2, MODEL_DIM, q_cols), MODEL_DIM),
        'w_key': weight(shared_keys[1], (2, MODEL_DIM, kv_cols), MODEL_DIM),
        'w_value': weight(shared_keys[2], (2, MODEL_DIM, kv_cols), MODEL_DIM),
        'w_out': weight(shared_keys[3], (2, q_cols, MODEL_DIM), q_cols),
        'w_gate': weight(shared_keys[4], (2, MODEL_DIM, FFN_DIM), MODEL_DIM),
        'w_up': weight(shared_keys[5], (2, MODEL_DIM, FFN_DIM), MODEL_DIM),
        'w_down': weight(shared_keys[6], (2, FFN_DIM, MODEL_DIM), FFN_DIM),
        'norm_gain': 0.3 * jax.random.normal(shared_keys[7], (2, 4, MODEL_DIM), jnp.float32),
        'qk_gain': 0.3 * jax.random.normal(shared_keys[8], (2, 2, HEAD_DIM), jnp.float32),
    }


def rms_scale(values, gain_vec):
    return values * lax.rsqrt(jnp.mean(values * values, axis=-1, keepdims=True) + NORM_EPS) * (1.0 + gain_vec)


def rotate(values, positions, rope_base, divisor):
    half_dim = values.shape[-1] // 2
    inv_freq = 1.0 / (rope_base ** (jnp.arange(0, 2 * half_dim, 2, dtype=jnp.float32) / (2 * half_dim)))
    angles = (positions.astype(jnp.float32) / divisor)[:, None] * inv_freq[None, :]
    angles = jnp.concatenate([angles, angles], axis=-1)[:, None, :]
    turned = jnp.concatenate([-values[..., half_dim:], values[..., :half_dim]], axis=-1)
    return values * jnp.cos(angles) + turned * jnp.sin(angles)


def attention(queries, key_all, value_all, query_pos, key_pos, key_ok, window):
    block_count = CHUNK_LEN // QUERY_BLOCK
    head_queries = jnp.transpose(queries.reshape(block_count, QUERY_BLOCK, KV_HEADS, GROUPS, HEAD_DIM), (2, 0, 1, 3, 4))
    pos_blocks = query_pos.reshape(block_count, QUERY_BLOCK)

    def per_head(head_args):
        block_queries, head_keys, head_values = head_args
        keys_f = head_keys.astype(jnp.float32)
        values_f = head_values.astype(jnp.float32)

        def per_block(block_args):
            one_block, block_pos = block_args
            scores = jnp.einsum('qgd,td->qgt', one_block.astype(jnp.float32), keys_f) * HEAD_DIM ** -0.5
            distance = block_pos[:, None] - key_pos[None, :]
            visible = key_ok[None, :] & (distance >= 0) & (distance < window)
            scores = jnp.where(visible[:, None, :], scores, -1e30)
            attn_prob = jax.nn.softmax(scores, axis=-1).astype(jnp.bfloat16)
            return jnp.einsum('qgt,td->qgd', attn_prob.astype(jnp.float32), values_f).astype(jnp.bfloat16)

        return lax.map(per_block, (block_queries, pos_blocks))

    head_out = lax.map(per_head, (head_queries, jnp.transpose(key_all, (1, 0, 2)), jnp.transpose(value_all, (1, 0, 2))))
    return jnp.transpose(head_out, (1, 2, 0, 3, 4)).reshape(CHUNK_LEN, NUM_HEADS * HEAD_DIM)


def decoder_layer(hidden, positions, layer_gains, qk_pair, w_query, w_key, w_value, w_out, w_gate, w_up, w_down, past_k, past_v, past_pos, past_ok, rope_base, divisor, window):
    normed = rms_scale(hidden.astype(jnp.float32), layer_gains[0]).astype(jnp.bfloat16)
    queries = jnp.dot(normed, w_query, preferred_element_type=jnp.float32).reshape(CHUNK_LEN, NUM_HEADS, HEAD_DIM)
    key_new = jnp.dot(normed, w_key, preferred_element_type=jnp.float32).reshape(CHUNK_LEN, KV_HEADS, HEAD_DIM)
    value_new = jnp.dot(normed, w_value, preferred_element_type=jnp.float32).astype(jnp.bfloat16).reshape(CHUNK_LEN, KV_HEADS, HEAD_DIM)
    queries = rotate(rms_scale(queries, qk_pair[0]), positions, rope_base, divisor).astype(jnp.bfloat16)
    key_new = rotate(rms_scale(key_new, qk_pair[1]), positions, rope_base, divisor).astype(jnp.bfloat16)
    key_all = jnp.concatenate([past_k, key_new], axis=0)
    value_all = jnp.concatenate([past_v, value_new], axis=0)
    key_pos = jnp.concatenate([past_pos, positions])
    key_ok = jnp.concatenate([past_ok, jnp.ones((CHUNK_LEN,), dtype=bool)])
    attn_out = attention(queries, key_all, value_all, positions, key_pos, key_ok, window)
    attn_proj = jnp.dot(attn_out, w_out, preferred_element_type=jnp.float32).astype(jnp.bfloat16)
    residual = (hidden.astype(jnp.float32) + rms_scale(attn_proj.astype(jnp.float32), layer_gains[1])).astype(jnp.bfloat16)
    normed = rms_scale(residual.astype(jnp.float32), layer_gains[2]).astype(jnp.bfloat16)
    gate_proj = jnp.dot(normed, w_gate, preferred_element_type=jnp.float32)
    up_proj = jnp.dot(normed, w_up, preferred_element_type=jnp.float32)
    hidden_act = (jax.nn.gelu(gate_proj, approximate=True) * up_proj).astype(jnp.bfloat16)
    down_proj = jnp.dot(hidden_act, w_down, preferred_element_type=jnp.float32).astype(jnp.bfloat16)
    layer_out = (residual.astype(jnp.float32) + rms_scale(down_proj.astype(jnp.float32), layer_gains[3])).astype(jnp.bfloat16)
    return layer_out, key_new, value_new


def reference(hidden, start_pos, k_local, v_local, k_global, v_global, w_query, w_key, w_value, w_out, w_gate, w_up, w_down, norm_gain, qk_gain):
    first_pos = start_pos[0]
    positions = first_pos + jnp.arange(CHUNK_LEN)
    slot_pos = first_pos - WINDOW + jnp.remainder(jnp.arange(WINDOW) - first_pos, WINDOW)
    middle, key_loc, value_loc = decoder_layer(hidden, positions, norm_gain[0], qk_gain[0], w_query[0], w_key[0], w_value[0], w_out[0], w_gate[0], w_up[0], w_down[0], k_local, v_local, slot_pos, jnp.ones((WINDOW,), dtype=bool), LOCAL_BASE, 1.0, WINDOW)
    cache_index = jnp.arange(CACHE_LEN)
    final_out, key_glob, value_glob = decoder_layer(middle, positions, norm_gain[1], qk_gain[1], w_query[1], w_key[1], w_value[1], w_out[1], w_gate[1], w_up[1], w_down[1], k_global, v_global, cache_index, cache_index < first_pos, GLOBAL_BASE, GLOBAL_DIV, CACHE_LEN + CHUNK_LEN + 1)
    return (final_out, key_loc, value_loc, key_glob, value_glob)
```

```python
import functools

import jax
import jax.numpy as jnp
from jax import lax
from jax.experimental import pallas as pl
from jax.experimental.pallas import tpu as pltpu
from jax.sharding import PartitionSpec as P

NORM_EPS = 1e-6
LOCAL_BASE = 10000.0
GLOBAL_BASE = 1000000.0
GLOBAL_DIV = 8.0
NEG_BIG = -1e30
HEAD = 256
TILE = 256
VMEM_LIMIT = 67_000_000
MESH = pl.DeviceIdType.MESH
F32 = jnp.float32
BF16 = jnp.bfloat16


def dot(a, b):
    return jnp.dot(a, b, preferred_element_type=F32)


def dot_t(a, b):
    return lax.dot_general(a, b, (((1,), (1,)), ((), ())), preferred_element_type=F32)


def unit_rms(values):
    return values * lax.rsqrt(jnp.mean(values * values, axis=-1, keepdims=True) + NORM_EPS)


def rope_tables(positions, rope_base, divisor):
    half = HEAD // 2
    inv_freq = 1.0 / (rope_base ** (jnp.arange(0, 2 * half, 2, dtype=F32) / (2 * half)))
    angles = (positions.astype(F32) / divisor)[:, None] * inv_freq[None, :]
    return jnp.cos(angles), jnp.sin(angles)


def enter(peers):
    barrier = pltpu.get_barrier_semaphore()
    for peer in peers:
        pl.semaphore_signal(barrier, inc=1, device_id=peer, device_id_type=MESH)
    pl.semaphore_wait(barrier, len(peers))


def front_kernel(layer, window, g_row, x_hbm, g_ref, qk_ref, cos_ref, sin_ref, wq_hbm, wk_hbm, wv_hbm, kc_hbm, vc_hbm, o_hbm, k_hbm, v_hbm, xv, h, wt, q_v, kall, vall, o_v, x_sem, w_sem, kv_sem, c_sem, s_sem, r_sem, o_sem):
    rows, dim = x_hbm.shape
    kv_cols = k_hbm.shape[1]
    n_kv = kv_cols // HEAD
    n_q = q_v.shape[1] // HEAD
    base = rows if window else 0
    n_tile = 2 * n_kv + n_q
    chunk = rows // 4

    def w_copies(j):
        return (
            (j < n_kv, wv_hbm, j, n_kv),
            ((j >= n_kv) & (j < 2 * n_kv), wk_hbm, j - n_kv, n_kv),
            ((j >= 2 * n_kv) & (j < n_tile), wq_hbm, j - 2 * n_kv, n_q),
        )

    def w_copy(w_hbm, i, slot):
        return pltpu.make_async_copy(w_hbm.at[layer, :, pl.ds(pl.multiple_of(i * HEAD, HEAD), HEAD)], wt.at[slot], w_sem.at[slot])

    def start_w(j):
        for cond, w_hbm, i, count in w_copies(j):
            pl.when(cond)(lambda w_hbm=w_hbm, i=i, count=count: w_copy(w_hbm, jnp.clip(i, 0, count - 1), j % 2).start())

    def wait_w(j):
        w_copy(wv_hbm, 0, j % 2).wait()

    x_dst = xv if window else h
    x_copies = [pltpu.make_async_copy(x_hbm.at[pl.ds(i * chunk, chunk)], x_dst.at[pl.ds(i * chunk, chunk)], x_sem.at[i]) for i in range(4)]
    for copy in x_copies:
        copy.start()
    start_w(jnp.int32(0))
    start_w(jnp.int32(1))
    if window:
        me = lax.axis_index('cp')
        size = lax.axis_size('cp')
        right = lax.rem(me + 1, size)
        left = lax.rem(me + size - 1, size)
        enter(({'cp': left}, {'cp': right}))
        first = me == 0
        c_copies = [pltpu.make_async_copy(kc_hbm, kall.at[pl.ds(0, rows)], c_sem.at[0]), pltpu.make_async_copy(vc_hbm, vall.at[pl.ds(0, rows)], c_sem.at[1])]
        for copy in c_copies:
            pl.when(first)(copy.start)
    for copy in x_copies:
        copy.wait()
    if window:
        def norm_rows(i, carry):
            part = pl.ds(pl.multiple_of(i * 16, 16), 16)
            h[part, :] = (unit_rms(xv[part, :].astype(F32)) * (1.0 + g_ref[g_row:g_row + 1, :])).astype(BF16)
            return carry
        lax.fori_loop(0, rows // 16, norm_rows, 0)

    def rope(acc, part, gain):
        scaled = unit_rms(acc) * gain
        cos = cos_ref[part, :]
        sin = sin_ref[part, :]
        low = scaled[:, :HEAD // 2]
        high = scaled[:, HEAD // 2:]
        return jnp.concatenate([low * cos - high * sin, high * cos + low * sin], axis=-1)

    def head_tile(j, finish_tile):
        wait_w(j)
        slot = j % 2

        def rows_step(i, carry):
            part = pl.ds(pl.multiple_of(i * chunk, chunk), chunk)
            finish_tile(i, part, dot(h[part, :], wt[slot]))
            return carry
        lax.fori_loop(0, 4, rows_step, 0)
        start_w(j + 2)

    def v_step(j, carry):
        def put(i, part, acc):
            vall[pl.ds(pl.multiple_of(base + i * chunk, chunk), chunk), pl.ds(pl.multiple_of(j * HEAD, HEAD), HEAD)] = acc.astype(BF16)
        head_tile(j, put)
        return carry
    lax.fori_loop(0, n_kv, v_step, 0)

    def k_step(j, carry):
        def put(i, part, acc):
            kall[pl.ds(pl.multiple_of(base + i * chunk, chunk), chunk), pl.ds(pl.multiple_of(j * HEAD, HEAD), HEAD)] = rope(acc, part, 1.0 + qk_ref[2 * layer + 1:2 * layer + 2, :]).astype(BF16)
        head_tile(j + n_kv, put)
        return carry
    lax.fori_loop(0, n_kv, k_step, 0)

    kv_out = [pltpu.make_async_copy(kall.at[pl.ds(base, rows)], k_hbm, kv_sem.at[0]), pltpu.make_async_copy(vall.at[pl.ds(base, rows)], v_hbm, kv_sem.at[1])]
    for copy in kv_out:
        copy.start()
    if window:
        sends = [pltpu.make_async_remote_copy(src_ref=buf.at[pl.ds(base, rows)], dst_ref=buf.at[pl.ds(0, rows)], send_sem=s_sem.at[i], recv_sem=r_sem.at[i], device_id={'cp': right}, device_id_type=MESH) for i, buf in enumerate((kall, vall))]
        last = me == size - 1
        for copy in sends:
            pl.when(jnp.logical_not(last))(copy.start)

    def q_step(j, carry):
        def put(i, part, acc):
            q_v[part, pl.ds(pl.multiple_of(j * HEAD, HEAD), HEAD)] = (rope(acc, part, 1.0 + qk_ref[2 * layer:2 * layer + 1, :]).astype(BF16).astype(F32) * (HEAD ** -0.5)).astype(BF16)
        head_tile(j + 2 * n_kv, put)
        return carry
    lax.fori_loop(0, n_q, q_step, 0)

    if not window:
        out = pltpu.make_async_copy(q_v, o_hbm, o_sem.at[0])
        out.start()
        for copy in kv_out:
            copy.wait()
        out.wait()
        return

    @pl.when(first)
    def _():
        for copy in c_copies:
            copy.wait()

    @pl.when(jnp.logical_not(first))
    def _():
        for copy in sends:
            copy.wait_recv()

    groups = n_q // n_kv
    span = rows + chunk

    def attend(i, carry):
        part = pl.ds(pl.multiple_of(i * chunk, chunk), chunk)
        keys = pl.ds(pl.multiple_of(i * chunk, chunk), span)
        row_id = lax.broadcasted_iota(jnp.int32, (chunk, span), 0)
        col_id = lax.broadcasted_iota(jnp.int32, (chunk, span), 1)
        seen = (col_id > row_id) & (col_id <= row_id + rows)
        for head in range(n_kv):
            key = kall[keys, head * HEAD:(head + 1) * HEAD]
            value = vall[keys, head * HEAD:(head + 1) * HEAD]
            for g in range(groups):
                cols = slice((head * groups + g) * HEAD, (head * groups + g + 1) * HEAD)
                scores = jnp.where(seen, dot_t(q_v[part, cols], key), NEG_BIG)
                top = jnp.max(scores, axis=-1, keepdims=True)
                prob = jnp.exp(scores - top)
                total = jnp.sum(prob, axis=-1, keepdims=True)
                o_v[part, cols] = (dot(prob.astype(BF16), value) / total).astype(BF16)
        return carry
    lax.fori_loop(0, 4, attend, 0)
    out = pltpu.make_async_copy(o_v, o_hbm, o_sem.at[0])
    out.start()

    @pl.when(jnp.logical_not(last))
    def _():
        for copy in sends:
            copy.wait_send()
    for copy in kv_out:
        copy.wait()
    out.wait()


def front(layer, window, g_row, x, gains, qk_gains, cos, sin, w_query, w_key, w_value, k_cache, v_cache, collective_id):
    rows, dim = x.shape
    q_cols = w_query.shape[2]
    kv_cols = w_key.shape[2]
    key_rows = 2 * rows if window else rows
    any_spec = pl.BlockSpec(memory_space=pl.ANY)
    vmem_spec = pl.BlockSpec(memory_space=pltpu.VMEM)
    x_rows = rows if window else 16
    return pl.pallas_call(
        functools.partial(front_kernel, layer, window, g_row),
        out_shape=(jax.ShapeDtypeStruct((rows, q_cols), BF16), jax.ShapeDtypeStruct((rows, kv_cols), BF16), jax.ShapeDtypeStruct((rows, kv_cols), BF16)),
        in_specs=[any_spec, vmem_spec, vmem_spec, vmem_spec, vmem_spec, any_spec, any_spec, any_spec, any_spec, any_spec],
        out_specs=(any_spec, any_spec, any_spec),
        scratch_shapes=[
            pltpu.VMEM((x_rows, dim), BF16),
            pltpu.VMEM((rows, dim), BF16),
            pltpu.VMEM((2, dim, HEAD), BF16),
            pltpu.VMEM((rows, q_cols), BF16),
            pltpu.VMEM((key_rows, kv_cols), BF16),
            pltpu.VMEM((key_rows, kv_cols), BF16),
            pltpu.VMEM((rows, q_cols) if window else (16, q_cols), BF16),
            pltpu.SemaphoreType.DMA((4,)),
            pltpu.SemaphoreType.DMA((2,)),
            pltpu.SemaphoreType.DMA((2,)),
            pltpu.SemaphoreType.DMA((2,)),
            pltpu.SemaphoreType.DMA((2,)),
            pltpu.SemaphoreType.DMA((2,)),
            pltpu.SemaphoreType.DMA((1,)),
        ],
        compiler_params=pltpu.CompilerParams(collective_id=collective_id if window else None, has_side_effects=window, vmem_limit_bytes=VMEM_LIMIT),
        name='front_window' if window else 'front_global',
    )(x, gains, qk_gains, cos, sin, w_query, w_key, w_value, k_cache, v_cache)


def global_kernel(key_block, p0_ref, q_ref, kown, vown, kall, vall, kn_hbm, vn_hbm, o_ref, kb, vb, kn, vn, m_ref, l_ref, acc_ref, b_sem, s_sem, r_sem, n_sem):
    rows, q_cols = q_ref.shape
    size, shard, kv_cols = kall.shape
    n_kv = kv_cols // HEAD
    groups = q_cols // kv_cols
    me = lax.axis_index('cp')
    mate = me + 1 - 2 * lax.rem(me, 2)
    across = lax.rem(me + 2, size)
    chunk = rows // 2
    blocks = size * shard // key_block
    per_shard = shard // key_block
    masked_blocks = -(-(shard // 2) // key_block)
    first_pos = p0_ref[0]

    def fetch(idx, op):
        b = lax.rem(idx, blocks)
        slot = lax.rem(idx, 2)
        s = b // per_shard
        part = pl.ds(pl.multiple_of(lax.rem(b, per_shard) * key_block, key_block), key_block)

        @pl.when(s == me)
        def _():
            for i, (src, dst) in enumerate(((kown, kb), (vown, vb))):
                getattr(pltpu.make_async_copy(src.at[part], dst.at[slot], b_sem.at[slot, i]), op)()

        @pl.when(s != me)
        def _():
            for i, (src, dst) in enumerate(((kall, kb), (vall, vb))):
                getattr(pltpu.make_async_copy(src.at[s, part], dst.at[slot], b_sem.at[slot, i]), op)()

    fetch(jnp.int32(0), 'start')
    own = [pltpu.make_async_copy(kn_hbm, kn.at[me], n_sem.at[0]), pltpu.make_async_copy(vn_hbm, vn.at[me], n_sem.at[1])]
    for copy in own:
        copy.start()
    enter(({'cp': mate}, {'cp': across}))

    def remote(src, dst, i, peer):
        return pltpu.make_async_remote_copy(src_ref=src, dst_ref=dst, send_sem=s_sem.at[i], recv_sem=r_sem.at[i], device_id={'cp': peer}, device_id_type=MESH)
    to_across = [remote(kn_hbm, kn.at[me], 0, across), remote(vn_hbm, vn.at[me], 1, across)]
    to_mate = [remote(kn_hbm, kn.at[me], 2, mate), remote(vn_hbm, vn.at[me], 3, mate)]
    relay = [remote(kn.at[across], kn.at[across], 4, mate), remote(vn.at[across], vn.at[across], 5, mate)]
    for copy in to_across + to_mate:
        copy.start()
    for copy in own:
        copy.wait()

    def block_step(c, keys, values, seen_of):
        part = pl.ds(pl.multiple_of(c * chunk, chunk), chunk)
        for head in range(n_kv):
            query = jnp.concatenate([q_ref[part, (head * groups + g) * HEAD:(head * groups + g + 1) * HEAD] for g in range(groups)], axis=0)
            key = keys(head)
            scores = dot_t(query, key)
            if seen_of is not None:
                scores = jnp.where(seen_of(scores.shape), scores, NEG_BIG)
            old = m_ref[head]
            new = jnp.maximum(old, jnp.max(scores, axis=-1, keepdims=True))
            decay = jnp.exp(old - new)
            prob = jnp.exp(scores - jnp.concatenate([new] * (scores.shape[1] // 128), axis=1))
            lanes = prob[:, :128]
            for i in range(1, scores.shape[1] // 128):
                lanes = lanes + prob[:, i * 128:(i + 1) * 128]
            l_ref[head] = l_ref[head] * decay + lanes
            m_ref[head] = new
            acc_ref[head] = acc_ref[head] * jnp.concatenate([decay] * (HEAD // 128), axis=1) + dot(prob.astype(BF16), values(head))

    def chunk_step(c, carry):
        m_ref[...] = jnp.full(m_ref.shape, NEG_BIG, F32)
        l_ref[...] = jnp.zeros(l_ref.shape, F32)
        acc_ref[...] = jnp.zeros(acc_ref.shape, F32)

        def cache_step(masked, b, carry):
            idx = c * blocks + b
            fetch(idx, 'wait')

            @pl.when(idx + 1 < 2 * blocks)
            def _():
                fetch(idx + 1, 'start')
            slot = lax.rem(idx, 2)

            def seen_of(shape):
                return lax.broadcasted_iota(jnp.int32, shape, 1) < first_pos - b * key_block
            block_step(c, lambda head: kb[slot, :, head * HEAD:(head + 1) * HEAD], lambda head: vb[slot, :, head * HEAD:(head + 1) * HEAD], seen_of if masked else None)
            return carry
        lax.fori_loop(0, blocks - masked_blocks, functools.partial(cache_step, False), 0)

        @pl.when(c == 0)
        def _():
            for copy in to_across:
                copy.wait()
            for copy in relay:
                copy.start()
        lax.fori_loop(blocks - masked_blocks, blocks, functools.partial(cache_step, True), 0)

        @pl.when(c == 0)
        def _():
            for copy in to_mate + relay:
                copy.wait()
        per_new = rows // key_block

        def new_slices(i):
            s = i // per_new
            part = pl.ds(pl.multiple_of(lax.rem(i, per_new) * key_block, key_block), key_block)
            return (lambda head: kn[s, part, head * HEAD:(head + 1) * HEAD], lambda head: vn[s, part, head * HEAD:(head + 1) * HEAD])

        def past_step(i, carry):
            keys, values = new_slices(i)
            block_step(c, keys, values, None)
            return carry
        lax.fori_loop(0, me * per_new, past_step, 0)

        def own_step(i, carry):
            keys, values = new_slices(me * per_new + i)

            def seen_of(shape):
                row_id = lax.rem(lax.broadcasted_iota(jnp.int32, shape, 0), chunk)
                return lax.broadcasted_iota(jnp.int32, shape, 1) - row_id <= c * chunk - i * key_block
            block_step(c, keys, values, seen_of)
            return carry
        lax.fori_loop(0, ((c + 1) * chunk + key_block - 1) // key_block, own_step, 0)

        part = pl.ds(pl.multiple_of(c * chunk, chunk), chunk)
        for head in range(n_kv):
            total = jnp.sum(l_ref[head], axis=-1, keepdims=True)
            result = (acc_ref[head] / total).astype(BF16)
            for g in range(groups):
                o_ref[part, (head * groups + g) * HEAD:(head * groups + g + 1) * HEAD] = result[g * chunk:(g + 1) * chunk]
        return carry
    lax.fori_loop(0, 2, chunk_step, 0)


def global_attention(first_pos, queries, k_own, v_own, k_all, v_all, k_new, v_new, collective_id):
    rows, q_cols = queries.shape
    size, shard, kv_cols = k_all.shape
    n_kv = kv_cols // HEAD
    groups = q_cols // kv_cols
    key_block = min(512, shard // 2, rows // 2)
    stack = rows // 2 * groups
    any_spec = pl.BlockSpec(memory_space=pl.ANY)
    vmem_spec = pl.BlockSpec(memory_space=pltpu.VMEM)
    return pl.pallas_call(
        functools.partial(global_kernel, key_block),
        out_shape=jax.ShapeDtypeStruct((rows, q_cols), BF16),
        in_specs=[pl.BlockSpec(memory_space=pltpu.SMEM), vmem_spec] + [any_spec] * 6,
        out_specs=vmem_spec,
        scratch_shapes=[
            pltpu.VMEM((2, key_block, kv_cols), BF16),
            pltpu.VMEM((2, key_block, kv_cols), BF16),
            pltpu.VMEM((size, rows, kv_cols), BF16),
            pltpu.VMEM((size, rows, kv_cols), BF16),
            pltpu.VMEM((n_kv, stack, 128), F32),
            pltpu.VMEM((n_kv, stack, 128), F32),
            pltpu.VMEM((n_kv, stack, HEAD), F32),
            pltpu.SemaphoreType.DMA((2, 2)),
            pltpu.SemaphoreType.DMA((6,)),
            pltpu.SemaphoreType.DMA((6,)),
            pltpu.SemaphoreType.DMA((2,)),
        ],
        compiler_params=pltpu.CompilerParams(collective_id=collective_id, has_side_effects=True, vmem_limit_bytes=VMEM_LIMIT),
        name='global_attention',
    )(first_pos, queries, k_own, v_own, k_all, v_all, k_new, v_new)


N_CHUNK = 4
N_SUB = 4
RECV_SLOTS = 4


def back_kernel(layer, gather, *refs):
    if gather:
        (o_hbm, x_hbm, g_ref, wo_hbm, wg_hbm, wu_hbm, wd_hbm, kown, vown, xo_hbm, ho_hbm, kall, vall) = refs[:13]
        refs = refs[13:]
    else:
        (o_hbm, x_hbm, g_ref, wo_hbm, wg_hbm, wu_hbm, wd_hbm, xo_hbm) = refs[:8]
        refs = refs[8:]
    (part, tot, xv, u, wo_v, o_v, hact, gu, dn, recv2, wo_sem, ld_sem, gu_sem, dn_sem, s1, s2s, s2r, s3, credit, out_sem) = refs[:20]
    rows, dim = x_hbm.shape
    ff = wg_hbm.shape[2]
    chunk = rows // N_CHUNK
    sub = chunk // N_SUB
    per = N_CHUNK * N_SUB
    n_ev = 2 * per
    n_dim = dim // TILE
    n_ff = ff // TILE
    tp = lax.axis_index('tp')
    outer = (tp == 0) | (tp == 3)
    inner = jnp.logical_not(outer)
    mate = tp + 1 - 2 * lax.rem(tp, 2)
    middle = 3 - tp

    def cols(t):
        return pl.ds(pl.multiple_of(t * TILE, TILE), TILE)

    def rows_of(n):
        return pl.ds(pl.multiple_of(lax.rem(n, per) * sub, sub), sub)

    def wo_copy(t):
        return pltpu.make_async_copy(wo_hbm.at[layer, :, cols(t)], wo_v.at[:, cols(t)], wo_sem.at[t])

    def gu_copies(i):
        slot = lax.rem(i, 2)
        t = lax.rem(i, n_ff)
        return [pltpu.make_async_copy(w.at[layer, :, cols(t)], gu.at[slot, k], gu_sem.at[slot, k]) for k, w in enumerate((wg_hbm, wu_hbm))]

    def dn_copy(i):
        slot = lax.rem(i, 2)
        return pltpu.make_async_copy(wd_hbm.at[layer, :, cols(lax.rem(i, n_dim))], dn.at[slot], dn_sem.at[slot])

    o_copy = pltpu.make_async_copy(o_hbm, o_v, ld_sem.at[0])
    x_copy = pltpu.make_async_copy(x_hbm, xv, ld_sem.at[1])
    o_copy.start()
    for t in range(n_dim):
        wo_copy(t).start()
    x_copy.start()
    for i in range(2):
        for copy in gu_copies(jnp.int32(i)):
            copy.start()
        dn_copy(jnp.int32(i)).start()

    peers = [{'tp': mate}, {'tp': middle}]
    if gather:
        g_s, g_r = refs[20:22]
        size = lax.axis_size('cp')
        cp = lax.axis_index('cp')
        near = cp + 1 - 2 * lax.rem(cp, 2)
        across = lax.rem(cp + 2, size)
        peers += [{'cp': near}, {'cp': across}]
    enter(peers)
    if gather:
        def remote(src, dst, i, peer):
            return pltpu.make_async_remote_copy(src_ref=src, dst_ref=dst, send_sem=g_s.at[i], recv_sem=g_r.at[i], device_id={'cp': peer}, device_id_type=MESH)
        to_across = [remote(kown, kall.at[cp], 0, across), remote(vown, vall.at[cp], 1, across)]
        to_near = [remote(kown, kall.at[cp], 2, near), remote(vown, vall.at[cp], 3, near)]
        relay = [remote(kall.at[across], kall.at[across], 4, near), remote(vall.at[across], vall.at[across], 5, near)]
        for copy in to_across + to_near:
            copy.start()

    def hop1(n):
        return pltpu.make_async_remote_copy(src_ref=part.at[rows_of(n)], dst_ref=tot.at[rows_of(n)], send_sem=s1.at[n], recv_sem=s1.at[n], device_id={'tp': mate}, device_id_type=MESH)

    def hop2(n):
        return pltpu.make_async_remote_copy(src_ref=part.at[rows_of(n)], dst_ref=recv2.at[lax.rem(n, RECV_SLOTS)], send_sem=s2s.at[n], recv_sem=s2r.at[n], device_id={'tp': middle}, device_id_type=MESH)

    def hop3(n):
        return pltpu.make_async_remote_copy(src_ref=tot.at[rows_of(n)], dst_ref=tot.at[rows_of(n)], send_sem=s3.at[n], recv_sem=s3.at[n], device_id={'tp': mate}, device_id_type=MESH)

    def out_copies(n):
        m = lax.rem(n, per)
        made = [pltpu.make_async_copy(xv.at[rows_of(n)], xo_hbm.at[rows_of(n)], out_sem.at[0, m])]
        if gather:
            made.append(pltpu.make_async_copy(u.at[rows_of(n)], ho_hbm.at[rows_of(n)], out_sem.at[1, m]))
        return made

    def send_chunk(first):
        @pl.when(outer)
        def _():
            for i in range(N_SUB):
                hop1(first + i).start()

    def normalize(n):
        start = lax.rem(n, per) * sub
        step = min(16, sub)

        @pl.when(n < per)
        def _():
            def body(i, carry):
                r = pl.ds(pl.multiple_of(start + i * step, step), step)
                x1 = (xv[r, :].astype(F32) + unit_rms(tot[r, :].astype(F32)) * (1.0 + g_ref[4 * layer + 1:4 * layer + 2, :])).astype(BF16)
                xv[r, :] = x1
                u[r, :] = (unit_rms(x1.astype(F32)) * (1.0 + g_ref[4 * layer + 2:4 * layer + 3, :])).astype(BF16)
                return carry
            lax.fori_loop(0, sub // step, body, 0)

        @pl.when(n >= per)
        def _():
            def body(i, carry):
                r = pl.ds(pl.multiple_of(start + i * step, step), step)
                x2 = (xv[r, :].astype(F32) + unit_rms(tot[r, :].astype(F32)) * (1.0 + g_ref[4 * layer + 3:4 * layer + 4, :])).astype(BF16)
                xv[r, :] = x2
                if gather:
                    u[r, :] = (unit_rms(x2.astype(F32)) * (1.0 + g_ref[4 * layer + 4:4 * layer + 5, :])).astype(BF16)
                return carry
            lax.fori_loop(0, sub // step, body, 0)
            for copy in out_copies(n):
                copy.start()

    def event(tick):
        @pl.when(inner)
        def _():
            n = tick

            @pl.when((n >= 0) & (n < n_ev))
            def _():
                hop1(n).wait_recv()
                r = rows_of(n)
                part[r, :] = (part[r, :].astype(F32) + tot[r, :].astype(F32)).astype(BF16)

                @pl.when(n >= RECV_SLOTS)
                def _():
                    pl.semaphore_wait(credit, 1)
            k = tick - 1

            @pl.when((k >= 0) & (k < n_ev))
            def _():
                hop2(k).wait_recv()
                hop2(k).wait_send()
                r = rows_of(k)
                tot[r, :] = (part[r, :].astype(F32) + recv2[lax.rem(k, RECV_SLOTS)].astype(F32)).astype(BF16)

                @pl.when(k < n_ev - RECV_SLOTS)
                def _():
                    pl.semaphore_signal(credit, inc=1, device_id={'tp': middle}, device_id_type=MESH)

            @pl.when((n >= 0) & (n < n_ev))
            def _():
                hop2(n).start()

            @pl.when((k >= 0) & (k < n_ev))
            def _():
                @pl.when(k >= 1)
                def _():
                    hop3(k - 1).wait_send()
                normalize(k)
                hop3(k).start()

        @pl.when(outer)
        def _():
            n = tick - 2

            @pl.when((n >= 0) & (n < n_ev))
            def _():
                hop1(n).wait_send()
                hop3(n).wait_recv()
                normalize(n)

    o_copy.wait()

    def wo_chunk(c, carry):
        r = pl.ds(pl.multiple_of(c * chunk, chunk), chunk)

        def tile(t, carry):
            @pl.when(c == 0)
            def _():
                wo_copy(t).wait()
            part[r, cols(t)] = dot(o_v[r, :], wo_v[:, cols(t)]).astype(BF16)
            return carry
        lax.fori_loop(0, n_dim, tile, 0)
        send_chunk(c * N_SUB)
        return carry
    lax.fori_loop(0, N_CHUNK, wo_chunk, 0)
    x_copy.wait()

    lead = N_SUB + 2

    def tick_only(tick, carry):
        event(tick)
        return carry
    lax.fori_loop(0, lead, tick_only, 0)
    ticks_per = N_SUB + 1
    tasks = n_ff + n_dim
    stride = -(-tasks // ticks_per)

    def ffn_chunk(c, carry):
        r = pl.ds(pl.multiple_of(c * chunk, chunk), chunk)

        def task(t, carry):
            @pl.when(t < n_ff)
            def _():
                i = c * n_ff + t
                for copy in gu_copies(i):
                    copy.wait()
                slot = lax.rem(i, 2)
                lhs = u[r, :]
                gate = dot(lhs, gu[slot, 0])
                up = dot(lhs, gu[slot, 1])
                hact[:, cols(t)] = (jax.nn.gelu(gate, approximate=True) * up).astype(BF16)

                @pl.when(i + 2 < N_CHUNK * n_ff)
                def _():
                    for copy in gu_copies(i + 2):
                        copy.start()

            @pl.when(t >= n_ff)
            def _():
                i = c * n_dim + t - n_ff
                dn_copy(i).wait()
                part[r, cols(t - n_ff)] = dot(hact[...], dn[lax.rem(i, 2)]).astype(BF16)

                @pl.when(i + 2 < N_CHUNK * n_dim)
                def _():
                    dn_copy(i + 2).start()

            @pl.when(lax.rem(t, stride) == stride - 1)
            def _():
                event(lead + c * ticks_per + t // stride)
            return carry
        lax.fori_loop(0, tasks, task, 0)
        send_chunk(per + c * N_SUB)
        return carry
    lax.fori_loop(0, N_CHUNK, ffn_chunk, 0)
    done = lead + N_CHUNK * (tasks // stride)
    if gather:
        for copy in to_across:
            copy.wait()
        for copy in relay:
            copy.start()
    lax.fori_loop(done, n_ev + 2, tick_only, 0)

    @pl.when(inner)
    def _():
        hop3(n_ev - 1).wait_send()

    def finish(m, carry):
        for copy in out_copies(m):
            copy.wait()
        return carry
    lax.fori_loop(0, per, finish, 0)
    if gather:
        for copy in to_near + relay:
            copy.wait()


def back(layer, attn_out, hidden, gains, w_out, w_gate, w_up, w_down, cache, collective_id):
    rows, dim = hidden.shape
    q_cols = attn_out.shape[1]
    ff = w_gate.shape[2]
    chunk = rows // N_CHUNK
    sub = chunk // N_SUB
    gather = cache is not None
    any_spec = pl.BlockSpec(memory_space=pl.ANY)
    vmem_spec = pl.BlockSpec(memory_space=pltpu.VMEM)
    n_ev = 2 * N_CHUNK * N_SUB
    args = [attn_out, hidden, gains, w_out, w_gate, w_up, w_down]
    outs = [jax.ShapeDtypeStruct((rows, dim), BF16)]
    scratch = [
        pltpu.VMEM((rows, dim), BF16),
        pltpu.VMEM((rows, dim), BF16),
        pltpu.VMEM((rows, dim), BF16),
        pltpu.VMEM((rows, dim), BF16),
        pltpu.VMEM((q_cols, dim), BF16),
        pltpu.VMEM((rows, q_cols), BF16),
        pltpu.VMEM((chunk, ff), BF16),
        pltpu.VMEM((2, 2, dim, TILE), BF16),
        pltpu.VMEM((2, ff, TILE), BF16),
        pltpu.VMEM((RECV_SLOTS, sub, dim), BF16),
        pltpu.SemaphoreType.DMA((dim // TILE,)),
        pltpu.SemaphoreType.DMA((2,)),
        pltpu.SemaphoreType.DMA((2, 2)),
        pltpu.SemaphoreType.DMA((2,)),
        pltpu.SemaphoreType.DMA((n_ev,)),
        pltpu.SemaphoreType.DMA((n_ev,)),
        pltpu.SemaphoreType.DMA((n_ev,)),
        pltpu.SemaphoreType.DMA((n_ev,)),
        pltpu.SemaphoreType.REGULAR,
        pltpu.SemaphoreType.DMA((2, N_CHUNK * N_SUB)),
    ]
    if gather:
        shard, kv_cols = cache[0].shape
        args += list(cache)
        outs += [jax.ShapeDtypeStruct((rows, dim), BF16)] + [jax.ShapeDtypeStruct((4, shard, kv_cols), BF16)] * 2
        scratch += [pltpu.SemaphoreType.DMA((6,)), pltpu.SemaphoreType.DMA((6,))]
    return pl.pallas_call(
        functools.partial(back_kernel, layer, gather),
        out_shape=tuple(outs),
        in_specs=[any_spec, any_spec, vmem_spec] + [any_spec] * (len(args) - 3),
        out_specs=tuple([any_spec] * len(outs)),
        scratch_shapes=scratch,
        compiler_params=pltpu.CompilerParams(collective_id=collective_id, has_side_effects=True, vmem_limit_bytes=VMEM_LIMIT),
        name='back_%d' % layer,
    )(*args)


def solution(mesh):
    row_spec = P(('dp', 'cp'), None)
    cache_spec = P(('dp', 'cp'), 'tp', None)
    window_spec = P('dp', 'tp', None)
    col_spec = P(None, None, 'tp')
    row_split = P(None, 'tp', None)
    replicated = P()

    def device_step(hidden, start_pos, k_local, v_local, k_global, v_global, w_query, w_key, w_value, w_out, w_gate, w_up, w_down, norm_gain, qk_gain):
        first_pos = start_pos[0]
        cp_index = lax.axis_index('cp')
        rows, dim = hidden.shape
        window = k_local.shape[0]
        flat = lambda a: a.reshape(a.shape[0], -1)
        positions = first_pos + cp_index * rows + jnp.arange(rows)
        gains = jnp.concatenate([norm_gain.reshape(8, dim), jnp.zeros((8, dim), F32)], axis=0)
        qk_gains = jnp.concatenate([qk_gain.reshape(4, HEAD), jnp.zeros((4, HEAD), F32)], axis=0)
        turn = jnp.remainder(first_pos, window)
        rolled = [lax.dynamic_slice_in_dim(jnp.concatenate([flat(a), flat(a)], axis=0), turn, window, axis=0) for a in (k_local, v_local)]
        cos, sin = rope_tables(positions, LOCAL_BASE, 1.0)
        attn, key_loc, value_loc = front(0, True, 0, hidden, gains, qk_gains, cos, sin, w_query, w_key, w_value, rolled[0], rolled[1], 0)
        cache = (flat(k_global), flat(v_global))
        middle, normed, k_all, v_all = back(0, attn, hidden, gains, w_out, w_gate, w_up, w_down, cache, 1)
        cos, sin = rope_tables(positions, GLOBAL_BASE, GLOBAL_DIV)
        queries, key_glob, value_glob = front(1, False, 4, normed, gains, qk_gains, cos, sin, w_query, w_key, w_value, rolled[0], rolled[1], None)
        attn = global_attention(start_pos, queries, cache[0], cache[1], k_all, v_all, key_glob, value_glob, 2)
        final, = back(1, attn, middle, gains, w_out, w_gate, w_up, w_down, None, 3)
        shaped = lambda a: a.reshape(rows, -1, HEAD)
        return final, shaped(key_loc), shaped(value_loc), shaped(key_glob), shaped(value_glob)

    return jax.shard_map(device_step, mesh=mesh, in_specs=(row_spec, P('dp'), window_spec, window_spec, cache_spec, cache_spec, col_spec, col_spec, col_spec, row_split, col_spec, col_spec, row_split, replicated, replicated), out_specs=(row_spec, cache_spec, cache_spec, cache_spec, cache_spec), check_vma=False)
```

```python
import functools

import jax
import jax.numpy as jnp
from jax import lax
from jax.experimental import pallas as pl
from jax.experimental.pallas import tpu as pltpu
from jax.sharding import PartitionSpec as P

NORM_EPS = 1e-6
LOCAL_BASE = 10000.0
GLOBAL_BASE = 1000000.0
GLOBAL_DIV = 8.0
NEG_BIG = -1e30
HEAD = 256
TILE = 256
VMEM_LIMIT = 67_000_000
MESH = pl.DeviceIdType.MESH
F32 = jnp.float32
BF16 = jnp.bfloat16


def dot(a, b):
    return jnp.dot(a, b, preferred_element_type=F32)


def dot_t(a, b):
    return lax.dot_general(a, b, (((1,), (1,)), ((), ())), preferred_element_type=F32)


def unit_rms(values):
    return values * lax.rsqrt(jnp.mean(values * values, axis=-1, keepdims=True) + NORM_EPS)


def rope_tables(positions, rope_base, divisor):
    half = HEAD // 2
    inv_freq = 1.0 / (rope_base ** (jnp.arange(0, 2 * half, 2, dtype=F32) / (2 * half)))
    angles = (positions.astype(F32) / divisor)[:, None] * inv_freq[None, :]
    return jnp.cos(angles), jnp.sin(angles)


def enter(peers):
    barrier = pltpu.get_barrier_semaphore()
    for peer in peers:
        pl.semaphore_signal(barrier, inc=1, device_id=peer, device_id_type=MESH)
    pl.semaphore_wait(barrier, len(peers))


N_CHUNK = 4
N_SUB = 4
RECV_SLOTS = 4


def spread(count, weights):
    total, seen, marks = sum(weights), 0, []
    for i, weight in enumerate(weights):
        seen += weight
        if seen * count >= total * (len(marks) + 1):
            marks.append(i)
    return marks


def layer_kernel(layer, names, *refs):
    r = dict(zip(names, refs))
    first_layer = layer == 0
    x_hbm, g_ref, qk_ref = (r[n] for n in ('x', 'gains', 'qk_gains'))
    cos_ref, sin_ref = (r['cos'], r['sin']) if first_layer else (r['top'], r['sums'])
    part, tot, xv, wt, dn, wo_v, qo, hact, recv2 = (r[n] for n in ('part', 'tot', 'xv', 'wt', 'dn', 'wo_v', 'qo', 'hact', 'recv2'))
    rows, dim = x_hbm.shape
    ff = r['w_gate'].shape[2]
    kv_cols = r['w_key'].shape[2]
    q_cols = r['w_query'].shape[2]
    n_kv, n_q = kv_cols // HEAD, q_cols // HEAD
    groups = n_q // n_kv
    chunk = rows // N_CHUNK
    sub = chunk // N_SUB
    per = N_CHUNK * N_SUB
    n_ev = 2 * per
    n_dim, n_ff = dim // TILE, ff // TILE
    tp, cp, size = lax.axis_index('tp'), lax.axis_index('cp'), lax.axis_size('cp')
    outer = (tp == 0) | (tp == 3)
    inner = jnp.logical_not(outer)
    mate = tp + 1 - 2 * lax.rem(tp, 2)
    middle = 3 - tp
    near = cp + 1 - 2 * lax.rem(cp, 2)
    across = lax.rem(cp + 2, size)
    right, left = lax.rem(cp + 1, size), lax.rem(cp + size - 1, size)

    def aligned(start, length):
        return pl.ds(pl.multiple_of(start, length), length)

    def cols(t):
        return aligned(t * TILE, TILE)

    def chunk_rows(c):
        return aligned(c * chunk, chunk)

    def rows_of(n):
        return aligned(lax.rem(n, per) * sub, sub)

    n_tile = 2 * n_kv + n_q

    def start_w(j):
        for low, high, w_hbm in ((0, n_kv, r['w_value']), (n_kv, 2 * n_kv, r['w_key']), (2 * n_kv, n_tile, r['w_query'])):
            @pl.when((j >= low) & (j < high))
            def _():
                slot = lax.rem(j, 4)
                pltpu.make_async_copy(w_hbm.at[layer, :, cols(jnp.clip(j - low, 0, high - low - 1))], wt.at[slot], r['w_sem'].at[slot]).start()

    def wait_w(j):
        slot = lax.rem(j, 4)
        pltpu.make_async_copy(r['w_value'].at[layer, :, cols(0)], wt.at[slot], r['w_sem'].at[slot]).wait()

    def wo_copy(t):
        return pltpu.make_async_copy(r['w_out'].at[layer, :, cols(t)], wo_v.at[:, cols(t)], r['wo_sem'].at[t])

    def gu_copies(i):
        slot, t = lax.rem(i, 2) * 2, lax.rem(i, n_ff)
        return [pltpu.make_async_copy(r[w].at[layer, :, cols(t)], wt.at[slot + k], r['w_sem'].at[slot + k]) for k, w in enumerate(('w_gate', 'w_up'))]

    def dn_copy(i):
        slot = lax.rem(i, 2)
        return pltpu.make_async_copy(r['w_down'].at[layer, :, cols(lax.rem(i, n_dim))], dn.at[slot], r['dn_sem'].at[slot])

    h_src = x_hbm if first_layer else r['h']
    h_dst = xv if first_layer else part
    h_copies = [pltpu.make_async_copy(h_src.at[pl.ds(i * chunk, chunk)], h_dst.at[pl.ds(i * chunk, chunk)], r['h_sem'].at[i]) for i in range(N_CHUNK)]
    h_copies[0].start()
    start_w(jnp.int32(0))
    for copy in h_copies[1:]:
        copy.start()
    for j in range(1, 4):
        start_w(jnp.int32(j))
    if not first_layer:
        t_copies = [pltpu.make_async_copy(r[src], dst, r['own_sem'].at[i]) for i, (src, dst) in enumerate((('cos', cos_ref), ('sin', sin_ref)))]
        for copy in t_copies:
            copy.start()

    peers = [{'tp': mate}, {'tp': middle}, {'cp': near}, {'cp': across}]
    if first_layer:
        peers += [{'cp': left}, {'cp': right}]
    enter(peers)

    def to_cp(src, dst, kind, i, peer):
        return pltpu.make_async_remote_copy(src_ref=src, dst_ref=dst, send_sem=r[kind + '_s'].at[i], recv_sem=r[kind + '_r'].at[i], device_id={'cp': peer}, device_id_type=MESH)

    if first_layer:
        is_first, is_last = cp == 0, cp == size - 1
        old_copies = [pltpu.make_async_copy(r[old], r[buf].at[pl.ds(0, rows)], r['old_sem'].at[i]) for i, (old, buf) in enumerate((('k_old', 'keys'), ('v_old', 'values')))]

        @pl.when(is_first)
        def _():
            for copy in old_copies:
                copy.start()
        for i, copy in enumerate(h_copies):
            copy.wait()

            def norm_rows(k, carry):
                these = aligned(i * chunk + k * 16, 16)
                part[these, :] = (unit_rms(xv[these, :].astype(F32)) * (1.0 + g_ref[0:1, :])).astype(BF16)
                return carry
            lax.fori_loop(0, chunk // 16, norm_rows, 0)
        base = rows
    else:
        for copy in h_copies + t_copies:
            copy.wait()
        base = 0

    def rope(acc, these, gain):
        scaled = unit_rms(acc) * gain
        cos, sin = cos_ref[these, :], sin_ref[these, :]
        low, high = scaled[:, :HEAD // 2], scaled[:, HEAD // 2:]
        return jnp.concatenate([low * cos - high * sin, high * cos + low * sin], axis=-1)

    def head_tile(j, put):
        wait_w(j)

        def rows_step(c, carry):
            these = chunk_rows(c)
            put(c, these, dot(part[these, :], wt[lax.rem(j, 4)]))
            return carry
        lax.fori_loop(0, N_CHUNK, rows_step, 0)
        start_w(j + 4)

    def v_step(j, carry):
        def put(c, these, acc):
            r['values'][aligned(base + c * chunk, chunk), cols(j)] = acc.astype(BF16)
        head_tile(j, put)
        return carry

    def k_step(j, carry):
        def put(c, these, acc):
            r['keys'][aligned(base + c * chunk, chunk), cols(j)] = rope(acc, these, 1.0 + qk_ref[2 * layer + 1:2 * layer + 2, :]).astype(BF16)
        head_tile(j + n_kv, put)
        return carry

    def q_step(j, carry):
        def put(c, these, acc):
            qo[these, cols(j)] = (rope(acc, these, 1.0 + qk_ref[2 * layer:2 * layer + 1, :]).astype(BF16).astype(F32) * (HEAD ** -0.5)).astype(BF16)
        head_tile(j + 2 * n_kv, put)
        return carry
    lax.fori_loop(0, n_kv, v_step, 0)
    lax.fori_loop(0, n_kv, k_step, 0)
    new_kv = [r[buf].at[pl.ds(base, rows)] for buf in ('keys', 'values')]
    kv_out = [pltpu.make_async_copy(src, r[dst], r['kv_sem'].at[i]) for i, (src, dst) in enumerate(zip(new_kv, ('k_new', 'v_new')))]
    if first_layer:
        sends = [to_cp(src, r[buf].at[pl.ds(0, rows)], 'n', i, right) for i, (src, buf) in enumerate(zip(new_kv, ('keys', 'values')))]

        @pl.when(jnp.logical_not(is_last))
        def _():
            for copy in sends:
                copy.start()
    else:
        alls = ('kn_all', 'vn_all')
        n_across = [to_cp(src, r[dst].at[cp], 'n', i, across) for i, (src, dst) in enumerate(zip(new_kv, alls))]
        n_near = [to_cp(src, r[dst].at[cp], 'n', 2 + i, near) for i, (src, dst) in enumerate(zip(new_kv, alls))]
        n_relay = [to_cp(r[dst].at[across], r[dst].at[across], 'n', 4 + i, near) for i, dst in enumerate(alls)]
        n_own = [pltpu.make_async_copy(src, r[dst].at[cp], r['own_sem'].at[i]) for i, (src, dst) in enumerate(zip(new_kv, alls))]
        for copy in n_across + n_near + n_own:
            copy.start()
    for copy in kv_out:
        copy.start()
    for t in range(n_dim):
        wo_copy(t).start()
    if not first_layer:
        x_copy = pltpu.make_async_copy(x_hbm, xv, r['x_sem'].at[0])
        x_copy.start()
    lax.fori_loop(0, n_q, q_step, 0)
    for i in range(2):
        for copy in gu_copies(jnp.int32(i)):
            copy.start()
        dn_copy(jnp.int32(i)).start()

    def to_tp(src, dst, send_sem, recv_sem, peer):
        return pltpu.make_async_remote_copy(src_ref=src, dst_ref=dst, send_sem=send_sem, recv_sem=recv_sem, device_id={'tp': peer}, device_id_type=MESH)

    def hop1(n):
        return to_tp(part.at[rows_of(n)], tot.at[rows_of(n)], r['s1'].at[n], r['s1'].at[n], mate)

    def hop2(n):
        return to_tp(part.at[rows_of(n)], recv2.at[lax.rem(n, RECV_SLOTS)], r['s2s'].at[n], r['s2r'].at[n], middle)

    def hop3(n):
        return to_tp(tot.at[rows_of(n)], tot.at[rows_of(n)], r['s3'].at[n], r['s3'].at[n], mate)

    def out_copies(n):
        made = [pltpu.make_async_copy(xv.at[rows_of(n)], r['x_out'].at[rows_of(n)], r['out_sem'].at[0, lax.rem(n, per)])]
        if first_layer:
            made.append(pltpu.make_async_copy(part.at[rows_of(n)], r['h_out'].at[rows_of(n)], r['out_sem'].at[1, lax.rem(n, per)]))
        return made

    def send_chunk(first):
        @pl.when(outer)
        def _():
            for i in range(N_SUB):
                hop1(first + i).start()

    def normalize(n):
        start = lax.rem(n, per) * sub
        step = min(16, sub)

        def update(these, row):
            value = (xv[these, :].astype(F32) + unit_rms(tot[these, :].astype(F32)) * (1.0 + g_ref[row:row + 1, :])).astype(BF16)
            xv[these, :] = value
            return value.astype(F32)

        @pl.when(n < per)
        def _():
            def body(i, carry):
                these = aligned(start + i * step, step)
                value = update(these, 4 * layer + 1)
                part[these, :] = (unit_rms(value) * (1.0 + g_ref[4 * layer + 2:4 * layer + 3, :])).astype(BF16)
                return carry
            lax.fori_loop(0, sub // step, body, 0)

        @pl.when(n >= per)
        def _():
            def body(i, carry):
                these = aligned(start + i * step, step)
                value = update(these, 4 * layer + 3)
                if first_layer:
                    part[these, :] = (unit_rms(value) * (1.0 + g_ref[4:5, :])).astype(BF16)
                return carry
            lax.fori_loop(0, sub // step, body, 0)
            for copy in out_copies(n):
                copy.start()

    def event(tick):
        n, k, m = tick, tick - 1, tick - 2

        @pl.when(inner)
        def _():
            @pl.when((n >= 0) & (n < n_ev))
            def _():
                hop1(n).wait_recv()
                these = rows_of(n)
                part[these, :] = (part[these, :].astype(F32) + tot[these, :].astype(F32)).astype(BF16)

                @pl.when(n >= RECV_SLOTS)
                def _():
                    pl.semaphore_wait(r['credit'], 1)

            @pl.when((k >= 0) & (k < n_ev))
            def _():
                hop2(k).wait_recv()
                hop2(k).wait_send()
                these = rows_of(k)
                tot[these, :] = (part[these, :].astype(F32) + recv2[lax.rem(k, RECV_SLOTS)].astype(F32)).astype(BF16)

                @pl.when(k < n_ev - RECV_SLOTS)
                def _():
                    pl.semaphore_signal(r['credit'], inc=1, device_id={'tp': middle}, device_id_type=MESH)

            @pl.when((n >= 0) & (n < n_ev))
            def _():
                hop2(n).start()

            @pl.when((k >= 1) & (k < n_ev))
            def _():
                hop3(k - 1).wait_send()

        @pl.when(outer & (m >= 0) & (m < n_ev))
        def _():
            hop1(m).wait_send()
            hop3(m).wait_recv()
        late = jnp.where(inner, k, m)

        @pl.when((late >= 0) & (late < n_ev))
        def _():
            normalize(late)

            @pl.when(inner)
            def _():
                hop3(late).start()

    def event_loop(low, high):
        def body(tick, carry):
            event(tick)
            return carry
        lax.fori_loop(low, high, body, 0)

    def project_chunk(c):
        these = chunk_rows(c)

        def tile(t, carry):
            @pl.when(c == 0)
            def _():
                wo_copy(t).wait()
            part[these, cols(t)] = dot(qo[these, :], wo_v[:, cols(t)]).astype(BF16)
            return carry
        lax.fori_loop(0, n_dim, tile, 0)
        send_chunk(c * N_SUB)

    if first_layer:
        @pl.when(is_first)
        def _():
            for copy in old_copies:
                copy.wait()

        @pl.when(jnp.logical_not(is_first))
        def _():
            for copy in sends:
                copy.wait_recv()
        caches = ('k_own', 'v_own')
        alls = ('k_all', 'v_all')
        c_across = [to_cp(r[src], r[dst].at[cp], 'g', i, across) for i, (src, dst) in enumerate(zip(caches, alls))]
        c_near = [to_cp(r[src], r[dst].at[cp], 'g', 2 + i, near) for i, (src, dst) in enumerate(zip(caches, alls))]
        c_relay = [to_cp(r[dst].at[across], r[dst].at[across], 'g', 4 + i, near) for i, dst in enumerate(alls)]

        @pl.when(jnp.logical_not(is_last))
        def _():
            for copy in sends:
                copy.wait_send()
        for copy in c_across + c_near:
            copy.start()
        span = rows + chunk

        def window_chunk(c, carry):
            these = chunk_rows(c)
            seen_keys = pl.ds(pl.multiple_of(c * chunk, chunk), span)
            row_id = lax.broadcasted_iota(jnp.int32, (chunk, span), 0)
            col_id = lax.broadcasted_iota(jnp.int32, (chunk, span), 1)
            seen = (col_id > row_id) & (col_id <= row_id + rows)
            for head in range(n_kv):
                key = r['keys'][seen_keys, head * HEAD:(head + 1) * HEAD]
                value = r['values'][seen_keys, head * HEAD:(head + 1) * HEAD]
                for g in range(groups):
                    these_cols = slice((head * groups + g) * HEAD, (head * groups + g + 1) * HEAD)
                    scores = jnp.where(seen, dot_t(qo[these, these_cols], key), NEG_BIG)
                    top = jnp.max(scores, axis=-1, keepdims=True)
                    prob = jnp.exp(scores - top)
                    total = jnp.sum(prob, axis=-1, keepdims=True)
                    qo[these, these_cols] = (dot(prob.astype(BF16), value) / total).astype(BF16)
            project_chunk(c)
            return carry
        lax.fori_loop(0, N_CHUNK, window_chunk, 0)
        next_tick = 6
        event_loop(0, next_tick)
    else:
        block = rows
        shard = r['k_own'].shape[0]
        per_shard = shard // block
        n_cache = size * per_shard
        n_mask = -(-(shard // 2) // block)
        n_full = n_cache - n_mask
        n_blocks = n_cache + cp + 1
        first_pos = r['first_pos'][0]
        stack = groups * chunk
        step = min(256, stack)
        scores_refs = (r['s_even'], r['s_odd'])

        def fetch(b, own, every, new, dst, sem, op):
            cache_id = jnp.where(b < n_mask, n_full + b, b - n_mask)
            s = cache_id // per_shard
            where = aligned(lax.rem(cache_id, per_shard) * block, block)

            @pl.when((b < n_cache) & (s == cp))
            def _():
                getattr(pltpu.make_async_copy(own.at[where], dst, sem), op)()

            @pl.when((b < n_cache) & (s != cp))
            def _():
                getattr(pltpu.make_async_copy(every.at[jnp.clip(s, 0, size - 1), where], dst, sem), op)()

            @pl.when(b >= n_cache)
            def _():
                getattr(pltpu.make_async_copy(new.at[jnp.clip(b - n_cache, 0, size - 1)], dst, sem), op)()

        def fetch_k(i, b, op):
            slot = lax.rem(i, 3)
            fetch(b, r['k_own'], r['k_all'], r['kn_all'], r['kb'].at[slot], r['kb_sem'].at[slot], op)

        def fetch_v(i, b, op):
            slot = lax.rem(i, 2)
            fetch(b, r['v_own'], r['v_all'], r['vn_all'], r['vb'].at[slot], r['vb_sem'].at[slot], op)

        def arrived():
            for copy in n_near + n_across:
                copy.wait()
            for copy in n_relay:
                copy.start()
            for copy in n_relay:
                copy.wait()
            for copy in n_own:
                copy.wait()

        def raw_scores(c, head, slot):
            query = jnp.concatenate([qo[chunk_rows(c), (head * groups + g) * HEAD:(head * groups + g + 1) * HEAD] for g in range(groups)], axis=0)
            scores_refs[head][...] = dot_t(query, r['kb'][slot, :, head * HEAD:(head + 1) * HEAD])

        def absorb(head, slot, seen_of):
            value = r['vb'][slot, :, head * HEAD:(head + 1) * HEAD]
            for low in range(0, stack, step):
                these = slice(low, low + step)
                scores = scores_refs[head][these, :]
                if seen_of is not None:
                    scores = jnp.where(seen_of(low, scores.shape), scores, NEG_BIG)
                state = slice(head * stack + low, head * stack + low + step)
                old = r['top'][state, :]
                new = jnp.maximum(old, jnp.max(scores, axis=-1, keepdims=True))
                decay = jnp.exp(old - new)
                prob = jnp.exp(scores - jnp.concatenate([new] * (block // 128), axis=1))
                lanes = prob[:, :128]
                for i in range(1, block // 128):
                    lanes = lanes + prob[:, i * 128:(i + 1) * 128]
                r['sums'][state, :] = r['sums'][state, :] * decay + lanes
                r['top'][state, :] = new
                r['acc'][head, these, :] = r['acc'][head, these, :] * jnp.concatenate([decay] * (HEAD // 128), axis=1) + dot(prob.astype(BF16), value)

        marks = [n_full * k // 9 for k in (2, 5, 8)]

        def attend_chunk(c, carry):
            start = c * n_blocks
            r['top'][...] = jnp.full(r['top'].shape, NEG_BIG, F32)
            r['sums'][...] = jnp.zeros(r['sums'].shape, F32)
            r['acc'][...] = jnp.zeros(r['acc'].shape, F32)

            @pl.when(c == 0)
            def _():
                fetch_k(0, 0, 'start')
                fetch_v(0, 0, 'start')
                fetch_k(1, 1, 'start')
                fetch_k(0, 0, 'wait')
            raw_scores(c, 0, lax.rem(start, 3))

            def block_step(seen_kind, b, carry):
                i = start + b
                fetch_v(i, b, 'wait')
                last = b == n_blocks - 1
                more = jnp.logical_not(last & (c == N_CHUNK - 1))

                @pl.when((c == 0) & (b + 2 == n_cache))
                def _():
                    arrived()

                @pl.when(more)
                def _():
                    fetch_k(i + 1, jnp.where(last, 0, b + 1), 'wait')
                    fetch_v(i + 1, jnp.where(last, 0, b + 1), 'start')

                @pl.when(jnp.logical_not((b >= n_blocks - 2) & (c == N_CHUNK - 1)))
                def _():
                    fetch_k(i + 2, jnp.where(b >= n_blocks - 2, b + 2 - n_blocks, b + 2), 'start')
                slot, later, v_slot = lax.rem(i, 3), lax.rem(i + 1, 3), lax.rem(i, 2)

                def seen_of(low, shape):
                    col_id = lax.broadcasted_iota(jnp.int32, shape, 1)
                    if seen_kind == 'cache':
                        return col_id < first_pos - (n_full + b) * block
                    row_id = lax.rem(low, chunk) + lax.rem(lax.broadcasted_iota(jnp.int32, shape, 0), chunk)
                    return col_id - row_id <= c * chunk
                seen = None if seen_kind is None else seen_of
                raw_scores(c, 1, slot)
                absorb(0, v_slot, seen)
                raw_scores(c, 0, later)
                absorb(1, v_slot, seen)
                if seen_kind is None:
                    at = b - n_mask
                    hit = (at == marks[0]) | (at == marks[1]) | (at == marks[2])

                    @pl.when(hit & (c > 0))
                    def _():
                        event((c - 1) * N_SUB + (at > marks[0]).astype(jnp.int32) + (at > marks[1]).astype(jnp.int32))
                return carry
            lax.fori_loop(0, n_mask, functools.partial(block_step, 'cache'), 0)
            lax.fori_loop(n_mask, n_cache + cp, functools.partial(block_step, None), 0)
            lax.fori_loop(n_cache + cp, n_blocks, functools.partial(block_step, 'own'), 0)
            these = chunk_rows(c)
            for head in range(n_kv):
                total = jnp.sum(r['sums'][head * stack:(head + 1) * stack, :], axis=-1, keepdims=True)
                result = (r['acc'][head] / total).astype(BF16)
                for g in range(groups):
                    qo[these, (head * groups + g) * HEAD:(head * groups + g + 1) * HEAD] = result[g * chunk:(g + 1) * chunk]
            project_chunk(c)

            @pl.when(c > 0)
            def _():
                event((c - 1) * N_SUB + 3)
            return carry
        x_copy.wait()
        lax.fori_loop(0, N_CHUNK, attend_chunk, 0)
        next_tick = (N_CHUNK - 1) * N_SUB

    tasks = n_ff + n_dim
    ffn_marks = spread(N_SUB, [2] * n_ff + [1] * n_dim)

    def ffn_chunk(c, carry):
        these = chunk_rows(c)

        def task(t, carry):
            @pl.when(t < n_ff)
            def _():
                i = c * n_ff + t
                for copy in gu_copies(i):
                    copy.wait()
                slot = lax.rem(i, 2) * 2
                lhs = part[these, :]
                gate = dot(lhs, wt[slot])
                up = dot(lhs, wt[slot + 1])
                hact[:, cols(t)] = (jax.nn.gelu(gate, approximate=True) * up).astype(BF16)

                @pl.when(i + 2 < N_CHUNK * n_ff)
                def _():
                    for copy in gu_copies(i + 2):
                        copy.start()

            @pl.when(t >= n_ff)
            def _():
                i = c * n_dim + t - n_ff
                dn_copy(i).wait()
                part[these, cols(t - n_ff)] = dot(hact[...], dn[lax.rem(i, 2)]).astype(BF16)

                @pl.when(i + 2 < N_CHUNK * n_dim)
                def _():
                    dn_copy(i + 2).start()
            hit = t == ffn_marks[0]
            which = jnp.int32(0)
            for mark in ffn_marks[1:]:
                which = which + (t >= mark).astype(jnp.int32)
                hit = hit | (t == mark)

            @pl.when(hit)
            def _():
                event(next_tick + c * N_SUB + which)
            return carry
        lax.fori_loop(0, tasks, task, 0)
        send_chunk(per + c * N_SUB)
        return carry
    lax.fori_loop(0, N_CHUNK, ffn_chunk, 0)
    drain = next_tick + N_CHUNK * N_SUB
    if first_layer:
        event_loop(drain, n_ev - 3)
        for copy in c_across:
            copy.wait()
        for copy in c_relay:
            copy.start()
        event_loop(n_ev - 3, n_ev + 2)
    else:
        event_loop(drain, n_ev + 2)

    @pl.when(inner)
    def _():
        hop3(n_ev - 1).wait_send()

    def finish(m, carry):
        for copy in out_copies(m):
            copy.wait()
        return carry
    lax.fori_loop(0, per, finish, 0)
    for copy in kv_out:
        copy.wait()
    if first_layer:
        for copy in c_near + c_relay:
            copy.wait()


def run_layer(layer, ins, collective_id):
    rows, dim = ins['x'].shape
    q_cols, kv_cols, ff = ins['w_query'].shape[2], ins['w_key'].shape[2], ins['w_gate'].shape[2]
    shard = ins['k_own'].shape[0]
    first_layer = layer == 0
    chunk = rows // N_CHUNK
    sub = chunk // N_SUB
    n_ev = 2 * N_CHUNK * N_SUB
    groups, n_kv = q_cols // kv_cols, kv_cols // HEAD
    stack = groups * chunk
    in_vmem = ('gains', 'qk_gains', 'cos', 'sin') if first_layer else ('gains', 'qk_gains')

    def spec(name):
        if name == 'first_pos':
            return pl.BlockSpec(memory_space=pltpu.SMEM)
        return pl.BlockSpec(memory_space=pltpu.VMEM if name in in_vmem else pl.ANY)
    array = jax.ShapeDtypeStruct
    outs = {'x_out': array((rows, dim), BF16), 'k_new': array((rows, kv_cols), BF16), 'v_new': array((rows, kv_cols), BF16)}
    dma = pltpu.SemaphoreType.DMA
    scratch = {
        'part': pltpu.VMEM((rows, dim), BF16),
        'tot': pltpu.VMEM((rows, dim), BF16),
        'xv': pltpu.VMEM((rows, dim), BF16),
        'wt': pltpu.VMEM((4, dim, TILE), BF16),
        'dn': pltpu.VMEM((2, ff, TILE), BF16),
        'wo_v': pltpu.VMEM((q_cols, dim), BF16),
        'qo': pltpu.VMEM((rows, q_cols), BF16),
        'hact': pltpu.VMEM((chunk, ff), BF16),
        'recv2': pltpu.VMEM((RECV_SLOTS, sub, dim), BF16),
        'w_sem': dma((4,)), 'dn_sem': dma((2,)), 'wo_sem': dma((dim // TILE,)), 'h_sem': dma((N_CHUNK,)),
        'kv_sem': dma((2,)), 'n_s': dma((6,)), 'n_r': dma((6,)),
        's1': dma((n_ev,)), 's2s': dma((n_ev,)), 's2r': dma((n_ev,)), 's3': dma((n_ev,)),
        'credit': pltpu.SemaphoreType.REGULAR, 'out_sem': dma((2, n_ev // 2)),
    }
    key_rows = 2 * rows if first_layer else rows
    scratch |= {'keys': pltpu.VMEM((key_rows, kv_cols), BF16), 'values': pltpu.VMEM((key_rows, kv_cols), BF16)}
    if first_layer:
        outs |= {'h_out': array((rows, dim), BF16), 'k_all': array((4, shard, kv_cols), BF16), 'v_all': array((4, shard, kv_cols), BF16)}
        scratch |= {'old_sem': dma((2,)), 'g_s': dma((6,)), 'g_r': dma((6,))}
    else:
        outs |= {'kn_all': array((4, rows, kv_cols), BF16), 'vn_all': array((4, rows, kv_cols), BF16)}
        scratch |= {
            'kb': pltpu.VMEM((3, rows, kv_cols), BF16),
            'vb': pltpu.VMEM((2, rows, kv_cols), BF16),
            's_even': pltpu.VMEM((stack, rows), F32),
            's_odd': pltpu.VMEM((stack, rows), F32),
            'top': pltpu.VMEM((n_kv * stack, 128), F32),
            'sums': pltpu.VMEM((n_kv * stack, 128), F32),
            'acc': pltpu.VMEM((n_kv, stack, HEAD), F32),
            'kb_sem': dma((3,)), 'vb_sem': dma((2,)), 'own_sem': dma((2,)), 'x_sem': dma((1,)),
        }
    names = tuple(ins) + tuple(outs) + tuple(scratch)
    made = pl.pallas_call(
        functools.partial(layer_kernel, layer, names),
        out_shape=tuple(outs.values()),
        in_specs=[spec(name) for name in ins],
        out_specs=tuple(pl.BlockSpec(memory_space=pl.ANY) for _ in outs),
        scratch_shapes=list(scratch.values()),
        compiler_params=pltpu.CompilerParams(collective_id=collective_id, has_side_effects=True, vmem_limit_bytes=VMEM_LIMIT),
        name='layer_%d' % layer,
    )(*ins.values())
    return dict(zip(outs, made))


def solution(mesh):
    row_spec = P(('dp', 'cp'), None)
    cache_spec = P(('dp', 'cp'), 'tp', None)
    window_spec = P('dp', 'tp', None)
    col_spec = P(None, None, 'tp')
    row_split = P(None, 'tp', None)
    replicated = P()

    def device_step(hidden, start_pos, k_local, v_local, k_global, v_global, w_query, w_key, w_value, w_out, w_gate, w_up, w_down, norm_gain, qk_gain):
        first_pos = start_pos[0]
        cp_index = lax.axis_index('cp')
        rows, dim = hidden.shape
        window = k_local.shape[0]
        flat = lambda a: a.reshape(a.shape[0], -1)
        positions = first_pos + cp_index * rows + jnp.arange(rows)
        gains = jnp.concatenate([norm_gain.reshape(8, dim), jnp.zeros((8, dim), F32)], axis=0)
        qk_gains = jnp.concatenate([qk_gain.reshape(4, HEAD), jnp.zeros((4, HEAD), F32)], axis=0)
        turn = jnp.remainder(first_pos, window)
        rolled = [lax.dynamic_slice_in_dim(jnp.concatenate([flat(a), flat(a)], axis=0), turn, window, axis=0) for a in (k_local, v_local)]
        cache = (flat(k_global), flat(v_global))
        weights = {'w_query': w_query, 'w_key': w_key, 'w_value': w_value, 'w_out': w_out, 'w_gate': w_gate, 'w_up': w_up, 'w_down': w_down, 'k_own': cache[0], 'v_own': cache[1]}
        cos, sin = rope_tables(positions, LOCAL_BASE, 1.0)
        one = run_layer(0, {'x': hidden, 'gains': gains, 'qk_gains': qk_gains, 'cos': cos, 'sin': sin, 'k_old': rolled[0], 'v_old': rolled[1], **weights}, 0)
        cos, sin = rope_tables(positions, GLOBAL_BASE, GLOBAL_DIV)
        two = run_layer(1, {'first_pos': start_pos, 'x': one['x_out'], 'h': one['h_out'], 'gains': gains, 'qk_gains': qk_gains, 'cos': cos, 'sin': sin, 'k_all': one['k_all'], 'v_all': one['v_all'], **weights}, 1)
        shaped = lambda a: a.reshape(rows, -1, HEAD)
        return two['x_out'], shaped(one['k_new']), shaped(one['v_new']), shaped(two['k_new']), shaped(two['v_new'])

    return jax.shard_map(device_step, mesh=mesh, in_specs=(row_spec, P('dp'), window_spec, window_spec, cache_spec, cache_spec, col_spec, col_spec, col_spec, row_split, col_spec, col_spec, row_split, replicated, replicated), out_specs=(row_spec, cache_spec, cache_spec, cache_spec, cache_spec), check_vma=False)
```

```python
import functools
import types

import jax
import jax.numpy as jnp
from jax import lax
from jax.experimental import pallas as pl
from jax.experimental.pallas import tpu as pltpu
from jax.sharding import PartitionSpec as P

NORM_EPS = 1e-6
LOCAL_BASE = 10000.0
GLOBAL_BASE = 1000000.0
GLOBAL_DIV = 8.0
NEG_BIG = -1e30
HEAD = 256
TILE = 256
VMEM_LIMIT = 67_000_000
MESH = pl.DeviceIdType.MESH
F32 = jnp.float32
BF16 = jnp.bfloat16


def dot(a, b):
    return jnp.dot(a, b, preferred_element_type=F32)


def dot_t(a, b):
    return lax.dot_general(a, b, (((1,), (1,)), ((), ())), preferred_element_type=F32)


def unit_rms(values):
    return values * lax.rsqrt(jnp.mean(values * values, axis=-1, keepdims=True) + NORM_EPS)


def rope_tables(first, rows, rope_base, divisor):
    half, step = HEAD // 2, 32
    inv_freq = 1.0 / (rope_base ** (jnp.arange(0, 2 * half, 2, dtype=F32) / (2 * half)))
    fine = (jnp.arange(step).astype(F32) / divisor)[:, None] * inv_freq[None, :]
    coarse = ((first + jnp.arange(0, rows, step)).astype(F32) / divisor)[:, None] * inv_freq[None, :]
    cos_f, sin_f, cos_c, sin_c = lax.optimization_barrier((jnp.cos(fine)[None], jnp.sin(fine)[None], jnp.cos(coarse)[:, None], jnp.sin(coarse)[:, None]))
    return (cos_c * cos_f - sin_c * sin_f).reshape(rows, half), (sin_c * cos_f + cos_c * sin_f).reshape(rows, half)


def enter(peers):
    for peer in peers:
        pl.semaphore_signal(pltpu.get_barrier_semaphore(), inc=1, device_id=peer, device_id_type=MESH)


def entered(peers):
    pl.semaphore_wait(pltpu.get_barrier_semaphore(), len(peers))


N_CHUNK = 4
N_SUB = 4
RECV_SLOTS = 4
LAG = 2
W_SLOTS = 6
D_SLOTS = 3
O_TILES = 3


def begin(copy):
    copy.start()


def end(copy):
    copy.wait()


def spread(count, weights):
    total, seen, marks = sum(weights), 0, []
    for i, weight in enumerate(weights):
        seen += weight
        if seen * count >= total * (len(marks) + 1):
            marks.append(i)
    return marks


def layers_kernel(names, *refs):
    r = types.SimpleNamespace(**dict(zip(names, refs)))
    x_hbm, g_ref, qk_ref = r.x, r.gains, r.qk_gains
    part, tot, xv, wt, dn, qo, hact, recv2 = r.part, r.tot, r.xv, r.wt, r.dn, r.qo, r.hact, r.recv2
    keys, values, top, sums, acc_ref = r.keys, r.values, r.top, r.sums, r.acc
    rows, dim = x_hbm.shape
    ff = r.w_gate.shape[2]
    kv_cols = r.w_key.shape[2]
    q_cols = r.w_query.shape[2]
    n_kv, n_q = kv_cols // HEAD, q_cols // HEAD
    groups = n_q // n_kv
    chunk = rows // N_CHUNK
    sub = chunk // N_SUB
    per = N_CHUNK * N_SUB
    n_ev = 2 * per
    n_tick = n_ev + LAG
    n_dim, n_ff = dim // TILE, ff // TILE
    tp, cp, size = lax.axis_index('tp'), lax.axis_index('cp'), lax.axis_size('cp')
    outer = (tp == 0) | (tp == 3)
    inner = jnp.logical_not(outer)
    mate = tp + 1 - 2 * lax.rem(tp, 2)
    middle = 3 - tp
    near = cp + 1 - 2 * lax.rem(cp, 2)
    across = lax.rem(cp + 2, size)
    far = lax.rem(near + 2, size)
    right = lax.rem(cp + 1, size)
    is_first, is_last = cp == 0, cp == size - 1

    def aligned(start, length):
        return pl.ds(pl.multiple_of(start, length), length)

    def cols(t):
        return aligned(t * TILE, TILE)

    def row_start(c):
        return (N_CHUNK - 1 - c) * chunk

    def chunk_rows(c):
        return aligned(row_start(c), chunk)

    def sub_start(n):
        m = lax.rem(n, per)
        return row_start(m // N_SUB) + lax.rem(m, N_SUB) * sub

    def rows_of(n):
        return aligned(sub_start(n), sub)

    n_tile = 2 * n_kv + n_q

    def start_w(layer, j):
        for low, high, w_hbm in ((0, n_kv, r.w_value), (n_kv, 2 * n_kv, r.w_key), (2 * n_kv, n_tile, r.w_query)):
            @pl.when((j >= low) & (j < high))
            def _():
                slot = lax.rem(j, W_SLOTS)
                pltpu.make_async_copy(w_hbm.at[layer, :, cols(jnp.clip(j - low, 0, high - low - 1))], wt.at[slot], r.w_sem.at[slot]).start()

    def wait_w(layer, j):
        slot = lax.rem(j, W_SLOTS)
        pltpu.make_async_copy(r.w_value.at[layer, :, cols(0)], wt.at[slot], r.w_sem.at[slot]).wait()

    per_slot = dim // q_cols
    places = W_SLOTS * per_slot

    def wo_place(k):
        place = lax.rem(k, places)
        return wt.at[place // per_slot, aligned(lax.rem(place, per_slot) * q_cols, q_cols)], r.wo_sem.at[place]

    def wo_copy(layer, k):
        dst, sem = wo_place(k)
        return pltpu.make_async_copy(r.w_out.at[layer, :, cols(lax.rem(k, n_dim))], dst, sem)

    def start_wo(layer):
        def body(k, carry):
            wo_copy(layer, k).start()
            return carry
        lax.fori_loop(0, places, body, 0)

    def gu_copies(layer, i):
        slot, t = lax.rem(i, W_SLOTS // 2) * 2, lax.rem(i, n_ff)
        return [pltpu.make_async_copy(w.at[layer, :, cols(t)], wt.at[slot + k], r.w_sem.at[slot + k]) for k, w in enumerate((r.w_gate, r.w_up))]

    def dn_copy(layer, i):
        slot = lax.rem(i, D_SLOTS)
        return pltpu.make_async_copy(r.w_down.at[layer, :, cols(lax.rem(i, n_dim))], dn.at[slot], r.dn_sem.at[slot])

    def start_gu(layer):
        for i in range(W_SLOTS // 2):
            for copy in gu_copies(layer, jnp.int32(i)):
                copy.start()

    def start_dn(layer):
        for i in range(D_SLOTS):
            dn_copy(layer, jnp.int32(i)).start()

    peers = [{'tp': mate}, {'tp': middle}, {'cp': near}, {'cp': across}, {'cp': far}]
    enter(peers)
    x_copies = [pltpu.make_async_copy(x_hbm.at[pl.ds(i * chunk, chunk)], xv.at[pl.ds(i * chunk, chunk)], r.x_sem.at[i]) for i in range(N_CHUNK)]
    x_copies[0].start()
    start_w(0, jnp.int32(0))
    for copy in x_copies[1:]:
        copy.start()
    for j in range(1, W_SLOTS):
        start_w(0, jnp.int32(j))
    half = n_kv * groups * chunk
    cos_ref, sin_ref = top.at[pl.ds(0, half)], sums.at[pl.ds(0, half)]
    t_copies = [pltpu.make_async_copy(table, dst, r.t_sem.at[i]) for i, (table, dst) in enumerate(((r.cos_local, cos_ref), (r.sin_local, sin_ref)))]
    for copy in t_copies:
        copy.start()
    start_dn(0)
    old_copies = [pltpu.make_async_copy(old, buf.at[pl.ds(0, rows)], r.old_sem.at[i]) for i, (old, buf) in enumerate(((r.k_old, keys), (r.v_old, values)))]

    @pl.when(is_first)
    def _():
        for copy in old_copies:
            copy.start()

    def to_cp(src, dst, sems, i, peer):
        return pltpu.make_async_remote_copy(src_ref=src, dst_ref=dst, send_sem=sems[0].at[i], recv_sem=sems[1].at[i], device_id={'cp': peer}, device_id_type=MESH)

    block = rows
    shard = r.k_own.shape[0]
    per_shard = shard // block
    own_names = ((r.k_own, r.k_all), (r.v_own, r.v_all))
    c_near = [to_cp(src, dst.at[cp], (r.c_near_s, r.c_near_r), i, near) for i, (src, dst) in enumerate(own_names)]

    def c_across(i):
        where = aligned(i * block, block)
        return [to_cp(src.at[where], dst.at[cp, where], (r.c_across_s, r.c_across_r), 2 * i + k, across) for k, (src, dst) in enumerate(own_names)]

    def c_relay(i):
        where = aligned(i * block, block)
        return [to_cp(dst.at[across, where], dst.at[across, where], (r.c_relay_s, r.c_relay_r), 2 * i + k, near) for k, (src, dst) in enumerate(own_names)]
    def rope(acc, cos, sin, gain):
        scaled = unit_rms(acc) * gain
        low, high = scaled[:, :HEAD // 2], scaled[:, HEAD // 2:]
        return jnp.concatenate([low * cos - high * sin, high * cos + low * sin], axis=-1)

    def as_query(value):
        return (value.astype(BF16).astype(F32) * (HEAD ** -0.5)).astype(BF16)

    for i in range(N_CHUNK):
        x_copies[i].wait()

        def norm_rows(k, carry):
            these = aligned(i * chunk + k * 32, 32)
            part[these, :] = (unit_rms(xv[these, :].astype(F32)) * (1.0 + g_ref[0:1, :])).astype(BF16)
            return carry
        lax.fori_loop(0, chunk // 32, norm_rows, 0)
    for copy in t_copies:
        copy.wait()

    tall = 2 * chunk

    def local_tile(j, put):
        wait_w(0, j)

        def rows_step(c, carry):
            these = aligned(c * tall, tall)
            put(c, these, dot(part[these, :], wt[lax.rem(j, W_SLOTS)]))
            return carry
        lax.fori_loop(0, rows // tall, rows_step, 0)
        start_w(0, j + W_SLOTS)

    def v_step(j, carry):
        def put(c, these, acc):
            values[aligned(rows + c * tall, tall), cols(j)] = acc.astype(BF16)
        local_tile(j, put)
        return carry

    def k_step(j, carry):
        def put(c, these, acc):
            keys[aligned(rows + c * tall, tall), cols(j)] = rope(acc, cos_ref[these, :], sin_ref[these, :], 1.0 + qk_ref[1:2, :]).astype(BF16)
        local_tile(j + n_kv, put)
        return carry

    def q_step(j, carry):
        def put(c, these, acc):
            qo[these, cols(j)] = as_query(rope(acc, cos_ref[these, :], sin_ref[these, :], 1.0 + qk_ref[0:1, :]))
        local_tile(j + 2 * n_kv, put)
        return carry
    lax.fori_loop(0, n_kv, v_step, 0)
    lax.fori_loop(0, n_kv, k_step, 0)

    def window_sends(c):
        return [to_cp(buf.at[aligned(rows + row_start(c), chunk)], buf.at[chunk_rows(c)], (r.w_s, r.w_r), 2 * c + i, right) for i, buf in enumerate((keys, values))]

    entered(peers)

    @pl.when(jnp.logical_not(is_last))
    def _():
        for c in range(N_CHUNK):
            for copy in window_sends(c):
                copy.start()
    for copy in c_near:
        copy.start()

    def across_start(i, carry):
        for copy in c_across(i):
            copy.start()
        return carry
    lax.fori_loop(0, per_shard, across_start, 0)
    kv_out = [pltpu.make_async_copy(buf.at[pl.ds(rows, rows)], dst, r.kv_sem.at[i]) for i, (buf, dst) in enumerate(((keys, r.k_new_0), (values, r.v_new_0)))]
    for copy in kv_out:
        copy.start()
    lax.fori_loop(0, n_q, q_step, 0)
    start_wo(0)

    def to_tp(src, dst, send_sem, recv_sem, peer):
        return pltpu.make_async_remote_copy(src_ref=src, dst_ref=dst, send_sem=send_sem, recv_sem=recv_sem, device_id={'tp': peer}, device_id_type=MESH)

    def hop1(n):
        return to_tp(part.at[rows_of(n)], tot.at[rows_of(n)], r.s1.at[n], r.s1.at[n], mate)

    def hop2(n):
        return to_tp(part.at[rows_of(n)], recv2.at[lax.rem(n, RECV_SLOTS)], r.s2s.at[n], r.s2r.at[n], middle)

    def hop3(n):
        return to_tp(tot.at[rows_of(n)], tot.at[rows_of(n)], r.s3.at[n], r.s3.at[n], mate)

    def out_copy(n):
        return pltpu.make_async_copy(xv.at[rows_of(n)], r.x_out.at[rows_of(n)], r.out_sem.at[lax.rem(n, per)])

    def send_chunk(first):
        @pl.when(outer)
        def _():
            for i in range(N_SUB):
                hop1(first + i).start()

    def normalize(layer, n):
        start = sub_start(n)
        step = min(32, sub)
        kind = n // per

        def body(i, carry):
            these = aligned(start + i * step, step)
            value = (xv[these, :].astype(F32) + unit_rms(tot[these, :].astype(F32)) * (1.0 + g_ref[pl.ds(4 * layer + 1 + 2 * kind, 1), :])).astype(BF16)
            xv[these, :] = value
            part[these, :] = (unit_rms(value.astype(F32)) * (1.0 + g_ref[pl.ds(4 * layer + 2 + 2 * kind, 1), :])).astype(BF16)
            return carry
        lax.fori_loop(0, sub // step, body, 0)

        @pl.when((layer == 1) & (kind == 1))
        def _():
            out_copy(n).start()

    def event(clock):
        layer = clock // n_tick
        n = lax.rem(clock, n_tick)
        k, m = n - 1, n - LAG

        @pl.when(inner)
        def _():
            @pl.when(n < n_ev)
            def _():
                hop1(n).wait_recv()
                these = rows_of(n)
                part[these, :] = (part[these, :].astype(F32) + tot[these, :].astype(F32)).astype(BF16)

                @pl.when((n >= RECV_SLOTS) | (layer == 1))
                def _():
                    pl.semaphore_wait(r.credit, 1)
                hop2(n).start()

            @pl.when((k >= 0) & (k < n_ev))
            def _():
                hop2(k).wait_recv()
                hop2(k).wait_send()
                these = rows_of(k)
                tot[these, :] = (part[these, :].astype(F32) + recv2[lax.rem(k, RECV_SLOTS)].astype(F32)).astype(BF16)

                @pl.when((k < n_ev - RECV_SLOTS) | (layer == 0))
                def _():
                    pl.semaphore_signal(r.credit, inc=1, device_id={'tp': middle}, device_id_type=MESH)

            @pl.when((k >= 2) & (k <= n_ev))
            def _():
                hop3(k - 2).wait_send()

            @pl.when(k == n_ev)
            def _():
                hop3(n_ev - 1).wait_send()

        @pl.when(outer & (m >= 0))
        def _():
            hop1(m).wait_send()
            hop3(m).wait_recv()
        late = jnp.where(inner, k, m)

        @pl.when((late >= 0) & (late < n_ev))
        def _():
            normalize(layer, late)

            @pl.when(inner)
            def _():
                hop3(late).start()
        piece = n - 14

        @pl.when((layer == 0) & (piece >= 0) & (piece < per_shard * 2))
        def _():
            i = piece // 2

            @pl.when(lax.rem(piece, 2) == 0)
            def _():
                c_across(i)[0].wait_recv()
                c_relay(i)[0].start()

            @pl.when(lax.rem(piece, 2) == 1)
            def _():
                c_across(i)[1].wait_recv()
                c_relay(i)[1].start()

    def event_loop(low, high):
        def body(clock, carry):
            event(clock)
            return carry
        lax.fori_loop(low, high, body, 0)

    def project_chunk(layer, c):
        these = chunk_rows(c)

        def tile(t, carry):
            first = c * n_dim + t * O_TILES
            for i in range(O_TILES):
                wo_copy(layer, first + i).wait()
            for i in range(O_TILES):
                part[these, cols(t * O_TILES + i)] = dot(qo[these, :], wo_place(first + i)[0][...]).astype(BF16)
            for i in range(O_TILES):
                @pl.when(first + i + places < N_CHUNK * n_dim)
                def _():
                    wo_copy(layer, first + i + places).start()
            return carry
        lax.fori_loop(0, n_dim // O_TILES, tile, 0)
        send_chunk(c * N_SUB)

    @pl.when(is_first)
    def _():
        for copy in old_copies:
            copy.wait()
    span = rows + chunk

    def window_chunk(c, carry):
        @pl.when(jnp.logical_not(is_first))
        def _():
            for copy in window_sends(c):
                copy.wait_recv()
        these = chunk_rows(c)
        seen_keys = pl.ds(pl.multiple_of(row_start(c), chunk), span)
        row_id = lax.broadcasted_iota(jnp.int32, (chunk, span), 0)
        col_id = lax.broadcasted_iota(jnp.int32, (chunk, span), 1)
        seen = (col_id > row_id) & (col_id <= row_id + rows)
        def one_head(n, carry):
            kv = cols(n // groups)
            scores = jnp.where(seen, dot_t(qo[these, cols(n)], keys[seen_keys, kv]), NEG_BIG)
            best = jnp.max(scores, axis=-1, keepdims=True)
            prob = jnp.exp(scores - best)
            total = jnp.sum(prob, axis=-1, keepdims=True)
            qo[these, cols(n)] = (dot(prob.astype(BF16), values[seen_keys, kv]) / total).astype(BF16)
            return carry
        lax.fori_loop(0, n_q, one_head, 0)
        project_chunk(0, c)

        @pl.when(c > 0)
        def _():
            event(c - 1)
        return carry
    lax.fori_loop(0, N_CHUNK, window_chunk, 0)
    start_gu(0)

    @pl.when(jnp.logical_not(is_last))
    def _():
        for c in range(N_CHUNK):
            for copy in window_sends(c):
                copy.wait_send()
    for copy in kv_out:
        copy.wait()

    def feed_forward(layer, clock):
        marks = spread(N_SUB, [2] * n_ff + [1] * n_dim)

        def ffn_chunk(c, carry):
            these = chunk_rows(c)

            def task(t, carry):
                @pl.when(t < n_ff)
                def _():
                    i = c * n_ff + t
                    for copy in gu_copies(layer, i):
                        copy.wait()
                    slot = lax.rem(i, W_SLOTS // 2) * 2
                    lhs = part[these, :]
                    gate = dot(lhs, wt[slot])
                    up = dot(lhs, wt[slot + 1])
                    hact[:, cols(t)] = (jax.nn.gelu(gate, approximate=True) * up).astype(BF16)

                    @pl.when(i + W_SLOTS // 2 < N_CHUNK * n_ff)
                    def _():
                        for copy in gu_copies(layer, i + W_SLOTS // 2):
                            copy.start()

                @pl.when(t >= n_ff)
                def _():
                    i = c * n_dim + t - n_ff
                    dn_copy(layer, i).wait()
                    part[these, cols(t - n_ff)] = dot(hact[...], dn[lax.rem(i, D_SLOTS)]).astype(BF16)

                    @pl.when(i + D_SLOTS < N_CHUNK * n_dim)
                    def _():
                        dn_copy(layer, i + D_SLOTS).start()
                hit = t == marks[0]
                which = jnp.int32(0)
                for mark in marks[1:]:
                    which = which + (t >= mark).astype(jnp.int32)
                    hit = hit | (t == mark)

                @pl.when(hit)
                def _():
                    event(clock + c * N_SUB + which)
                return carry
            lax.fori_loop(0, n_ff + n_dim, task, 0)
            send_chunk(per + c * N_SUB)
            return carry
        lax.fori_loop(0, N_CHUNK, ffn_chunk, 0)
    lead = N_SUB + LAG
    event_loop(N_CHUNK - 1, lead)
    feed_forward(0, lead)
    start_dn(1)

    def turn_copies(c):
        return [pltpu.make_async_copy(table.at[chunk_rows(c)], r.turn.at[i], r.t_sem.at[i]) for i, table in enumerate((r.cos_global, r.sin_global))]

    def start_project(c):
        for copy in turn_copies(c):
            copy.start()
        for j in range(W_SLOTS):
            start_w(1, jnp.int32(j))
    start_project(0)

    new_names = ((r.k_all_1, r.k_new_1), (r.v_all_1, r.v_new_1))

    def new_sends(c):
        buf = lax.rem(c, 2)
        return [to_cp(r.fresh.at[buf, i], dst.at[cp, chunk_rows(c)], (r.n_s, r.n_r), c * 6 + 2 * k + i, peer) for k, peer in enumerate((across, far, near)) for i, (dst, _) in enumerate(new_names)]

    def new_local(c):
        buf = lax.rem(c, 2)
        return [pltpu.make_async_copy(r.fresh.at[buf, i], place, r.own_sem.at[buf, 2 * i + k]) for i, (every, mine) in enumerate(new_names) for k, place in enumerate((every.at[cp, chunk_rows(c)], mine.at[chunk_rows(c)]))]

    def free_fresh(c):
        for copy in new_sends(c):
            copy.wait_send()
        for copy in new_local(c):
            copy.wait()

    def global_project(c):
        these = chunk_rows(c)
        buf = lax.rem(c, 2)
        @pl.when(c >= 2)
        def _():
            free_fresh(c - 2)
        for copy in turn_copies(c):
            copy.wait()

        def tile(j):
            wait_w(1, j)
            return dot(part[these, :], wt[lax.rem(j, W_SLOTS)])

        def gv_step(j, carry):
            r.fresh[buf, 1, :, cols(j)] = tile(j).astype(BF16)
            start_w(1, j + W_SLOTS)
            return carry

        def gk_step(j, carry):
            r.fresh[buf, 0, :, cols(j)] = rope(tile(j + n_kv), r.turn[0], r.turn[1], 1.0 + qk_ref[3:4, :]).astype(BF16)
            start_w(1, j + n_kv + W_SLOTS)
            return carry

        def gq_step(j, carry):
            qo[these, cols(j)] = as_query(rope(tile(j + 2 * n_kv), r.turn[0], r.turn[1], 1.0 + qk_ref[2:3, :]))
            start_w(1, j + 2 * n_kv + W_SLOTS)
            return carry
        lax.fori_loop(0, n_kv, gv_step, 0)
        lax.fori_loop(0, n_kv, gk_step, 0)
        for copy in new_sends(c) + new_local(c):
            copy.start()
        lax.fori_loop(0, n_q, gq_step, 0)

        @pl.when(c + 1 < N_CHUNK)
        def _():
            start_project(c + 1)

    n_pass = 2 * per_shard
    n_mask = -(-(shard // 2) // block)
    first_pos = r.first_pos[0]
    stack = groups * chunk
    step = min(256, stack)
    scores_refs = (r.s_even, r.s_odd)
    pair = cp // 2

    def pass_size(p):
        return jnp.where(p == 2, cp + 1, n_pass)

    def shard_of(p, b):
        return 2 * lax.rem(pair + p, 2) + lax.rem(b // per_shard, 2)

    def fetch(p, b, own, every, new, dst, sem, op):
        s = shard_of(p, b)
        where = aligned(lax.rem(b, per_shard) * block, block)

        @pl.when((p < 2) & (s == cp))
        def _():
            op(pltpu.make_async_copy(own.at[where], dst, sem))

        @pl.when((p < 2) & (s != cp))
        def _():
            op(pltpu.make_async_copy(every.at[s, where], dst, sem))

        @pl.when(p == 2)
        def _():
            op(pltpu.make_async_copy(new.at[lax.rem(b, size)], dst, sem))

    def fetch_k(p, b, op):
        slot = lax.rem(b, 3)
        fetch(p, b, r.k_own, r.k_all, r.k_all_1, keys.at[aligned(slot * block, block)], r.kb_sem.at[slot], op)

    def fetch_v(p, b, op):
        slot = lax.rem(b, 2)
        fetch(p, b, r.v_own, r.v_all, r.v_all_1, values.at[aligned(slot * block, block)], r.vb_sem.at[slot], op)

    def begin_pass(p):
        fetch_k(p, 0, begin)
        fetch_v(p, 0, begin)

        @pl.when(pass_size(p) > 1)
        def _():
            fetch_k(p, 1, begin)

    def raw_scores(c, head, slot):
        query = jnp.concatenate([qo[chunk_rows(c), (head * groups + g) * HEAD:(head * groups + g + 1) * HEAD] for g in range(groups)], axis=0)
        scores_refs[head][...] = dot_t(query, keys[aligned(slot * block, block), head * HEAD:(head + 1) * HEAD])

    def state(c, head, low, length):
        return aligned(lax.rem(c, 2) * half + head * stack + low, length)

    def absorb(c, head, slot, bound):
        value = values[aligned(slot * block, block), head * HEAD:(head + 1) * HEAD]
        for low in range(0, stack, step):
            scores = scores_refs[head][low:low + step, :]
            if bound is not None:
                limit, by_row = bound
                row_id = lax.rem(low, chunk) + lax.rem(lax.broadcasted_iota(jnp.int32, scores.shape, 0), chunk)
                scores = jnp.where(lax.broadcasted_iota(jnp.int32, scores.shape, 1) < limit + by_row * row_id, scores, NEG_BIG)
            these = state(c, head, low, step)
            old = top[these, :]
            new = jnp.maximum(old, jnp.max(scores, axis=-1, keepdims=True))
            decay = jnp.exp(old - new)
            prob = jnp.exp(scores - jnp.concatenate([new] * (block // 128), axis=1))
            lanes = prob[:, :128]
            for i in range(1, block // 128):
                lanes = lanes + prob[:, i * 128:(i + 1) * 128]
            sums[these, :] = sums[these, :] * decay + lanes
            top[these, :] = new
            acc_ref[these, :] = acc_ref[these, :] * jnp.concatenate([decay] * (HEAD // 128), axis=1) + dot(prob.astype(BF16), value)

    def job_step(j, carry):
        second = j // 6
        c = (1 - second) * lax.rem(j, 2) + second * (j // 3)
        p = (1 - second) * (j // 2) + second * lax.rem(j, 3)

        @pl.when((j < 2) | (j == 3))
        def _():
            low = j - j // 3

            def body(i, carry):
                before = lead + 16 + 3 * i + 2 * (i // 2) - 2 * (i // 3)
                event_loop(before, before + 1 + 2 * (i // 3))
                global_project(i)
                return carry
            lax.fori_loop(low, low + 1 + j // 3, body, 0)

            @pl.when(j == 3)
            def _():
                start_wo(1)

        @pl.when(p == 0)
        def _():
            for ref, value in ((top, NEG_BIG), (sums, 0.0), (acc_ref, 0.0)):
                ref[state(c, 0, 0, half), :] = jnp.full((half, ref.shape[1]), value, F32)
        count = pass_size(p)
        n_free = jnp.where(p == 2, cp, n_pass - n_mask)
        base = jnp.where(second == 1, n_tick + 1 + 5 * ((j - 6) // 3) + 2 * lax.rem(j, 3), jnp.where(j == 5, n_tick, lead + 17 + 3 * j - j // 2))
        fetch_k(p, 0, end)
        raw_scores(c, 0, 0)

        def block_step(masked, b, carry):
            fetch_v(p, b, end)

            @pl.when(b + 1 < count)
            def _():
                fetch_k(p, b + 1, end)
                fetch_v(p, b + 1, begin)

            @pl.when(b + 2 < count)
            def _():
                fetch_k(p, b + 2, begin)
            bound = None
            if masked:
                limit = jnp.where(p == 2, row_start(c) + 1, jnp.where(shard_of(p, b) == size - 1, first_pos - (size - 1) * shard - lax.rem(b, per_shard) * block, block))
                bound = (limit, jnp.where(p == 2, 1, 0))
            slot, later, v_slot = lax.rem(b, 3), lax.rem(b + 1, 3), lax.rem(b, 2)
            raw_scores(c, 1, slot)
            absorb(c, 0, v_slot, bound)
            raw_scores(c, 0, later)
            absorb(c, 1, v_slot, bound)
            if not masked:
                @pl.when((b == (n_pass - n_mask) // 2) & (p < 2) & (j != 3))
                def _():
                    event(base)
            return carry
        lax.fori_loop(0, n_free, functools.partial(block_step, False), 0)
        lax.fori_loop(n_free, count, functools.partial(block_step, True), 0)

        @pl.when(j == 1)
        def _():
            def body(i, carry):
                for copy in c_relay(i):
                    copy.wait_recv()
                return carry
            lax.fori_loop(0, per_shard, body, 0)

        @pl.when(j == 3)
        def _():
            free_fresh(2)
            free_fresh(3)

            def body(i, carry):
                for copy in new_sends(i):
                    copy.wait_recv()
                return carry
            lax.fori_loop(0, N_CHUNK, body, 0)

        @pl.when(j < 11)
        def _():
            after = j + 1
            begin_pass((1 - after // 6) * (after // 2) + (after // 6) * lax.rem(after, 3))

        @pl.when(p == 2)
        def _():
            these = chunk_rows(c)
            for head in range(n_kv):
                whole = state(c, head, 0, stack)
                total = jnp.sum(sums[whole, :], axis=-1, keepdims=True)
                result = (acc_ref[whole, :] / total).astype(BF16)
                for g in range(groups):
                    qo[these, (head * groups + g) * HEAD:(head * groups + g + 1) * HEAD] = result[g * chunk:(g + 1) * chunk]
            project_chunk(1, c)

        @pl.when((j != 3) & (j != 4))
        def _():
            event(base + jnp.where(p < 2, 1, 0))
        return carry
    for copy in c_near:
        copy.wait()
    begin_pass(jnp.int32(0))
    lax.fori_loop(0, 12, job_step, 0)
    start_gu(1)
    clock = n_tick + 11
    feed_forward(1, clock)
    event_loop(clock + N_CHUNK * N_SUB, 2 * n_tick)

    def finish(m, carry):
        out_copy(m).wait()
        return carry
    lax.fori_loop(0, per, finish, 0)

    def gathered(i, carry):
        for copy in c_across(i) + c_relay(i):
            copy.wait_send()
        return carry
    lax.fori_loop(0, per_shard, gathered, 0)


def run_layers(ins, collective_id):
    rows, dim = ins['x'].shape
    q_cols, kv_cols, ff = ins['w_query'].shape[2], ins['w_key'].shape[2], ins['w_gate'].shape[2]
    shard = ins['k_own'].shape[0]
    chunk = rows // N_CHUNK
    sub = chunk // N_SUB
    n_ev = 2 * N_CHUNK * N_SUB
    groups, n_kv = q_cols // kv_cols, kv_cols // HEAD
    stack = groups * chunk
    pieces = 2 * (shard // rows)

    def spec(name):
        if name == 'first_pos':
            return pl.BlockSpec(memory_space=pltpu.SMEM)
        return pl.BlockSpec(memory_space=pltpu.VMEM if name in ('gains', 'qk_gains') else pl.ANY)
    array = jax.ShapeDtypeStruct
    made = array((rows, kv_cols), BF16)
    outs = dict(x_out=array((rows, dim), BF16), k_new_0=made, v_new_0=made, k_new_1=made, v_new_1=made)
    outs |= dict(k_all=array((4, shard, kv_cols), BF16), v_all=array((4, shard, kv_cols), BF16), k_all_1=array((4, rows, kv_cols), BF16), v_all_1=array((4, rows, kv_cols), BF16))
    dma = pltpu.SemaphoreType.DMA
    scratch = dict(
        part=pltpu.VMEM((rows, dim), BF16),
        tot=pltpu.VMEM((rows, dim), BF16),
        xv=pltpu.VMEM((rows, dim), BF16),
        wt=pltpu.VMEM((W_SLOTS, dim, TILE), BF16),
        dn=pltpu.VMEM((D_SLOTS, ff, TILE), BF16),
        qo=pltpu.VMEM((rows, q_cols), BF16),
        hact=pltpu.VMEM((chunk, ff), BF16),
        recv2=pltpu.VMEM((RECV_SLOTS, sub, dim), BF16),
        keys=pltpu.VMEM((3 * rows, kv_cols), BF16),
        values=pltpu.VMEM((2 * rows, kv_cols), BF16),
        fresh=pltpu.VMEM((2, 2, chunk, kv_cols), BF16),
        turn=pltpu.VMEM((2, chunk, HEAD // 2), F32),
        s_even=pltpu.VMEM((stack, rows), F32),
        s_odd=pltpu.VMEM((stack, rows), F32),
        top=pltpu.VMEM((2 * n_kv * stack, 128), F32),
        sums=pltpu.VMEM((2 * n_kv * stack, 128), F32),
        acc=pltpu.VMEM((2 * n_kv * stack, HEAD), F32),
        w_sem=dma((W_SLOTS,)), wo_sem=dma((W_SLOTS * (dim // q_cols),)), dn_sem=dma((D_SLOTS,)), x_sem=dma((N_CHUNK,)), t_sem=dma((2,)), old_sem=dma((2,)),
        kv_sem=dma((2,)), own_sem=dma((2, 4)), kb_sem=dma((3,)), vb_sem=dma((2,)), out_sem=dma((n_ev // 2,)),
        w_s=dma((2 * N_CHUNK,)), w_r=dma((2 * N_CHUNK,)), n_s=dma((6 * N_CHUNK,)), n_r=dma((6 * N_CHUNK,)),
        c_near_s=dma((2,)), c_near_r=dma((2,)), c_across_s=dma((pieces,)), c_across_r=dma((pieces,)), c_relay_s=dma((pieces,)), c_relay_r=dma((pieces,)),
        s1=dma((n_ev,)), s2s=dma((n_ev,)), s2r=dma((n_ev,)), s3=dma((n_ev,)),
        credit=pltpu.SemaphoreType.REGULAR,
    )
    names = tuple(ins) + tuple(outs) + tuple(scratch)
    made = pl.pallas_call(
        functools.partial(layers_kernel, names),
        out_shape=tuple(outs.values()),
        in_specs=[spec(name) for name in ins],
        out_specs=tuple(pl.BlockSpec(memory_space=pl.ANY) for _ in outs),
        scratch_shapes=list(scratch.values()),
        compiler_params=pltpu.CompilerParams(collective_id=collective_id, has_side_effects=True, vmem_limit_bytes=VMEM_LIMIT),
        name='two_layers',
    )(*ins.values())
    return dict(zip(outs, made))


def solution(mesh):
    row_spec = P(('dp', 'cp'), None)
    cache_spec = P(('dp', 'cp'), 'tp', None)
    window_spec = P('dp', 'tp', None)
    col_spec = P(None, None, 'tp')
    row_split = P(None, 'tp', None)
    replicated = P()

    def device_step(hidden, start_pos, k_local, v_local, k_global, v_global, w_query, w_key, w_value, w_out, w_gate, w_up, w_down, norm_gain, qk_gain):
        first_pos = start_pos[0]
        cp_index = lax.axis_index('cp')
        rows, dim = hidden.shape
        window = k_local.shape[0]
        flat = lambda a: a.reshape(a.shape[0], -1)
        gains = jnp.concatenate([norm_gain.reshape(8, dim), jnp.zeros((8, dim), F32)], axis=0)
        qk_gains = jnp.concatenate([qk_gain.reshape(4, HEAD), jnp.zeros((4, HEAD), F32)], axis=0)
        turn = jnp.remainder(first_pos, window)
        rolled = [flat(lax.dynamic_slice_in_dim(jnp.concatenate([a, a], axis=0), turn, window, axis=0)) for a in (k_local, v_local)]
        cos_local, sin_local = rope_tables(first_pos + cp_index * rows, rows, LOCAL_BASE, 1.0)
        cos_global, sin_global = rope_tables(first_pos + cp_index * rows, rows, GLOBAL_BASE, GLOBAL_DIV)
        made = run_layers(dict(
            first_pos=start_pos, x=hidden, gains=gains, qk_gains=qk_gains,
            cos_local=cos_local, sin_local=sin_local, cos_global=cos_global, sin_global=sin_global,
            w_query=w_query, w_key=w_key, w_value=w_value, w_out=w_out, w_gate=w_gate, w_up=w_up, w_down=w_down,
            k_old=rolled[0], v_old=rolled[1], k_own=flat(k_global), v_own=flat(v_global),
        ), 0)
        shaped = lambda a: a.reshape(rows, -1, HEAD)
        return made['x_out'], shaped(made['k_new_0']), shaped(made['v_new_0']), shaped(made['k_new_1']), shaped(made['v_new_1'])

    return jax.shard_map(device_step, mesh=mesh, in_specs=(row_spec, P('dp'), window_spec, window_spec, cache_spec, cache_spec, col_spec, col_spec, col_spec, row_split, col_spec, col_spec, row_split, replicated, replicated), out_specs=(row_spec, cache_spec, cache_spec, cache_spec, cache_spec), check_vma=False)
```

```python
import functools
import types

import jax
import jax.numpy as jnp
from jax import lax
from jax.experimental import pallas as pl
from jax.experimental.pallas import tpu as pltpu
from jax.sharding import PartitionSpec as P

NORM_EPS = 1e-6
LOCAL_BASE = 10000.0
GLOBAL_BASE = 1000000.0
GLOBAL_DIV = 8.0
NEG_BIG = -1e30
HEAD = 256
TILE = 256
VMEM_LIMIT = 67_000_000
MESH = pl.DeviceIdType.MESH
F32 = jnp.float32
BF16 = jnp.bfloat16


def dot(a, b):
    return jnp.dot(a, b, preferred_element_type=F32)


def dot_t(a, b):
    return lax.dot_general(a, b, (((1,), (1,)), ((), ())), preferred_element_type=F32)


def unit_rms(values):
    return values * lax.rsqrt(jnp.mean(values * values, axis=-1, keepdims=True) + NORM_EPS)


def rope_tables(first, rows, rope_base, divisor):
    half, step = HEAD // 2, 32
    inv_freq = 1.0 / (rope_base ** (jnp.arange(0, 2 * half, 2, dtype=F32) / (2 * half)))
    fine = (jnp.arange(step).astype(F32) / divisor)[:, None] * inv_freq[None, :]
    coarse = ((first + jnp.arange(0, rows, step)).astype(F32) / divisor)[:, None] * inv_freq[None, :]
    cos_f, sin_f, cos_c, sin_c = lax.optimization_barrier((jnp.cos(fine)[None], jnp.sin(fine)[None], jnp.cos(coarse)[:, None], jnp.sin(coarse)[:, None]))
    return (cos_c * cos_f - sin_c * sin_f).reshape(rows, half), (sin_c * cos_f + cos_c * sin_f).reshape(rows, half)


def enter(peers):
    for peer in peers:
        pl.semaphore_signal(pltpu.get_barrier_semaphore(), inc=1, device_id=peer, device_id_type=MESH)


def entered(peers):
    pl.semaphore_wait(pltpu.get_barrier_semaphore(), len(peers))


N_CHUNK = 4
N_SUB = 4
RECV_SLOTS = 4
LAG = 2
W_SLOTS = 6
D_SLOTS = 3
O_TILES = 3


def spread(count, weights):
    total, seen, marks = sum(weights), 0, []
    for i, weight in enumerate(weights):
        seen += weight
        if seen * count >= total * (len(marks) + 1):
            marks.append(i)
    return marks


def layers_kernel(names, *refs):
    r = types.SimpleNamespace(**dict(zip(names, refs)))
    x_hbm, g_ref, qk_ref = r.x, r.gains, r.qk_gains
    part, tot, xv, wt, dn, qo, hact, recv2 = r.part, r.tot, r.xv, r.wt, r.dn, r.qo, r.hact, r.recv2
    keys, values, top, sums, acc_ref = r.keys, r.values, r.top, r.sums, r.acc
    rows, dim = x_hbm.shape
    ff = r.w_gate.shape[2]
    kv_cols = r.w_key.shape[2]
    q_cols = r.w_query.shape[2]
    n_kv, n_q = kv_cols // HEAD, q_cols // HEAD
    groups = n_q // n_kv
    chunk = rows // N_CHUNK
    sub = chunk // N_SUB
    per = N_CHUNK * N_SUB
    n_ev = 2 * per
    n_tick = n_ev + LAG
    n_dim, n_ff = dim // TILE, ff // TILE
    tp, cp, size = lax.axis_index('tp'), lax.axis_index('cp'), lax.axis_size('cp')
    outer = (tp == 0) | (tp == 3)
    inner = jnp.logical_not(outer)
    mate = tp + 1 - 2 * lax.rem(tp, 2)
    middle = 3 - tp
    near = cp + 1 - 2 * lax.rem(cp, 2)
    across = lax.rem(cp + 2, size)
    far = lax.rem(near + 2, size)
    right = lax.rem(cp + 1, size)
    is_first, is_last = cp == 0, cp == size - 1

    def aligned(start, length):
        return pl.ds(pl.multiple_of(start, length), length)

    def cols(t):
        return aligned(t * TILE, TILE)

    def row_start(c):
        return (N_CHUNK - 1 - c) * chunk

    def chunk_rows(c):
        return aligned(row_start(c), chunk)

    def sub_start(n):
        m = lax.rem(n, per)
        return row_start(m // N_SUB) + lax.rem(m, N_SUB) * sub

    def rows_of(n):
        return aligned(sub_start(n), sub)

    n_tile = 2 * n_kv + n_q

    def start_w(layer, j):
        for low, high, w_hbm in ((0, n_kv, r.w_value), (n_kv, 2 * n_kv, r.w_key), (2 * n_kv, n_tile, r.w_query)):
            @pl.when((j >= low) & (j < high))
            def _():
                slot = lax.rem(j, W_SLOTS)
                pltpu.make_async_copy(w_hbm.at[layer, :, cols(jnp.clip(j - low, 0, high - low - 1))], wt.at[slot], r.w_sem.at[slot]).start()

    def wait_w(layer, j):
        slot = lax.rem(j, W_SLOTS)
        pltpu.make_async_copy(r.w_value.at[layer, :, cols(0)], wt.at[slot], r.w_sem.at[slot]).wait()

    per_slot = dim // q_cols
    places = W_SLOTS * per_slot

    def wo_place(k):
        place = lax.rem(k, places)
        return wt.at[place // per_slot, aligned(lax.rem(place, per_slot) * q_cols, q_cols)], r.wo_sem.at[place]

    def wo_copy(layer, k):
        dst, sem = wo_place(k)
        return pltpu.make_async_copy(r.w_out.at[layer, :, cols(lax.rem(k, n_dim))], dst, sem)

    def start_wo(layer):
        def body(k, carry):
            wo_copy(layer, k).start()
            return carry
        lax.fori_loop(0, places, body, 0)

    def gu_copies(layer, i):
        slot, t = lax.rem(i, W_SLOTS // 2) * 2, lax.rem(i, n_ff)
        return [pltpu.make_async_copy(w.at[layer, :, cols(t)], wt.at[slot + k], r.w_sem.at[slot + k]) for k, w in enumerate((r.w_gate, r.w_up))]

    def dn_copy(layer, i):
        slot = lax.rem(i, D_SLOTS)
        return pltpu.make_async_copy(r.w_down.at[layer, :, cols(lax.rem(i, n_dim))], dn.at[slot], r.dn_sem.at[slot])

    def start_gu(layer):
        for i in range(W_SLOTS // 2):
            for copy in gu_copies(layer, jnp.int32(i)):
                copy.start()

    def start_dn(layer):
        for i in range(D_SLOTS):
            dn_copy(layer, jnp.int32(i)).start()

    peers = [{'tp': mate}, {'tp': middle}, {'cp': near}, {'cp': across}, {'cp': far}]
    enter(peers)
    x_copies = [pltpu.make_async_copy(x_hbm.at[pl.ds(i * chunk, chunk)], xv.at[pl.ds(i * chunk, chunk)], r.x_sem.at[i]) for i in range(N_CHUNK)]
    x_copies[0].start()
    start_w(0, jnp.int32(0))
    for copy in x_copies[1:]:
        copy.start()
    for j in range(1, W_SLOTS):
        start_w(0, jnp.int32(j))
    half = n_kv * groups * chunk
    cos_ref, sin_ref = top.at[pl.ds(0, half)], sums.at[pl.ds(0, half)]
    t_copies = [pltpu.make_async_copy(table, dst, r.t_sem.at[i]) for i, (table, dst) in enumerate(((r.cos_local, cos_ref), (r.sin_local, sin_ref)))]
    for copy in t_copies:
        copy.start()
    start_dn(0)
    old_copies = [pltpu.make_async_copy(old, buf.at[pl.ds(0, rows)], r.old_sem.at[i]) for i, (old, buf) in enumerate(((r.k_old, keys), (r.v_old, values)))]

    @pl.when(is_first)
    def _():
        for copy in old_copies:
            copy.start()

    def to_cp(src, dst, sems, i, peer):
        return pltpu.make_async_remote_copy(src_ref=src, dst_ref=dst, send_sem=sems[0].at[i], recv_sem=sems[1].at[i], device_id={'cp': peer}, device_id_type=MESH)

    block = rows
    shard = r.k_own.shape[0]
    per_shard = shard // block
    own_names = ((r.k_own, r.k_all), (r.v_own, r.v_all))
    c_near = [to_cp(src, dst.at[cp], (r.c_near_s, r.c_near_r), i, near) for i, (src, dst) in enumerate(own_names)]

    def c_across(i):
        where = aligned(i * block, block)
        return [to_cp(src.at[where], dst.at[cp, where], (r.c_across_s, r.c_across_r), 2 * i + k, across) for k, (src, dst) in enumerate(own_names)]

    def c_relay(i):
        where = aligned(i * block, block)
        return [to_cp(dst.at[across, where], dst.at[across, where], (r.c_relay_s, r.c_relay_r), 2 * i + k, near) for k, (src, dst) in enumerate(own_names)]
    def rope(acc, cos, sin, gain):
        scaled = unit_rms(acc) * gain
        low, high = scaled[:, :HEAD // 2], scaled[:, HEAD // 2:]
        return jnp.concatenate([low * cos - high * sin, high * cos + low * sin], axis=-1)

    def as_query(value):
        return (value.astype(BF16).astype(F32) * (HEAD ** -0.5)).astype(BF16)

    for i in range(N_CHUNK):
        x_copies[i].wait()

        def norm_rows(k, carry):
            these = aligned(i * chunk + k * 32, 32)
            part[these, :] = (unit_rms(xv[these, :].astype(F32)) * (1.0 + g_ref[0:1, :])).astype(BF16)
            return carry
        lax.fori_loop(0, chunk // 32, norm_rows, 0)
    for copy in t_copies:
        copy.wait()

    tall = 2 * chunk

    def local_tile(j, put):
        wait_w(0, j)

        def rows_step(c, carry):
            these = aligned(c * tall, tall)
            put(c, these, dot(part[these, :], wt[lax.rem(j, W_SLOTS)]))
            return carry
        lax.fori_loop(0, rows // tall, rows_step, 0)
        start_w(0, j + W_SLOTS)

    def v_step(j, carry):
        def put(c, these, acc):
            values[aligned(rows + c * tall, tall), cols(j)] = acc.astype(BF16)
        local_tile(j, put)
        return carry

    def k_step(j, carry):
        def put(c, these, acc):
            keys[aligned(rows + c * tall, tall), cols(j)] = rope(acc, cos_ref[these, :], sin_ref[these, :], 1.0 + qk_ref[1:2, :]).astype(BF16)
        local_tile(j + n_kv, put)
        return carry

    def q_step(j, carry):
        def put(c, these, acc):
            qo[these, cols(j)] = as_query(rope(acc, cos_ref[these, :], sin_ref[these, :], 1.0 + qk_ref[0:1, :]))
        local_tile(j + 2 * n_kv, put)
        return carry
    with jax.named_scope('kv0'):
        lax.fori_loop(0, n_kv, v_step, 0)
        lax.fori_loop(0, n_kv, k_step, 0)

    def window_sends(c):
        return [to_cp(buf.at[aligned(rows + row_start(c), chunk)], buf.at[chunk_rows(c)], (r.w_s, r.w_r), 2 * c + i, right) for i, buf in enumerate((keys, values))]

    with jax.named_scope('enter'):
        entered(peers)

    @pl.when(jnp.logical_not(is_last))
    def _():
        for c in range(N_CHUNK):
            for copy in window_sends(c):
                copy.start()
    for copy in c_near:
        copy.start()

    def across_start(i, carry):
        for copy in c_across(i):
            copy.start()
        return carry
    lax.fori_loop(0, per_shard, across_start, 0)
    kv_out = [pltpu.make_async_copy(buf.at[pl.ds(rows, rows)], dst, r.kv_sem.at[i]) for i, (buf, dst) in enumerate(((keys, r.k_new_0), (values, r.v_new_0)))]
    for copy in kv_out:
        copy.start()
    with jax.named_scope('q0'):
        lax.fori_loop(0, n_q, q_step, 0)
    start_wo(0)

    def to_tp(src, dst, send_sem, recv_sem, peer):
        return pltpu.make_async_remote_copy(src_ref=src, dst_ref=dst, send_sem=send_sem, recv_sem=recv_sem, device_id={'tp': peer}, device_id_type=MESH)

    def hop1(n):
        return to_tp(part.at[rows_of(n)], tot.at[rows_of(n)], r.s1.at[n], r.s1.at[n], mate)

    def hop2(n):
        return to_tp(part.at[rows_of(n)], recv2.at[lax.rem(n, RECV_SLOTS)], r.s2s.at[n], r.s2r.at[n], middle)

    def hop3(n):
        return to_tp(tot.at[rows_of(n)], tot.at[rows_of(n)], r.s3.at[n], r.s3.at[n], mate)

    def out_copy(n):
        return pltpu.make_async_copy(xv.at[rows_of(n)], r.x_out.at[rows_of(n)], r.out_sem.at[lax.rem(n, per)])

    def send_chunk(first):
        @pl.when(outer)
        def _():
            for i in range(N_SUB):
                hop1(first + i).start()

    def normalize(layer, n):
        start = sub_start(n)
        step = min(32, sub)
        kind = n // per

        def body(i, carry):
            these = aligned(start + i * step, step)
            value = (xv[these, :].astype(F32) + unit_rms(tot[these, :].astype(F32)) * (1.0 + g_ref[pl.ds(4 * layer + 1 + 2 * kind, 1), :])).astype(BF16)
            xv[these, :] = value
            part[these, :] = (unit_rms(value.astype(F32)) * (1.0 + g_ref[pl.ds(4 * layer + 2 + 2 * kind, 1), :])).astype(BF16)
            return carry
        lax.fori_loop(0, sub // step, body, 0)

        @pl.when((layer == 1) & (kind == 1))
        def _():
            out_copy(n).start()

    def event(clock):
        layer = clock // n_tick
        n = lax.rem(clock, n_tick)
        k, m = n - 1, n - LAG

        @pl.when(inner)
        def _():
            @pl.when(n < n_ev)
            def _():
                with jax.named_scope('w1'):
                    hop1(n).wait_recv()
                these = rows_of(n)
                part[these, :] = (part[these, :].astype(F32) + tot[these, :].astype(F32)).astype(BF16)

                @pl.when((n >= RECV_SLOTS) | (layer == 1))
                def _():
                    with jax.named_scope('wc'):
                        pl.semaphore_wait(r.credit, 1)
                hop2(n).start()

            @pl.when((k >= 0) & (k < n_ev))
            def _():
                with jax.named_scope('w2'):
                    hop2(k).wait_recv()
                    hop2(k).wait_send()
                these = rows_of(k)
                tot[these, :] = (part[these, :].astype(F32) + recv2[lax.rem(k, RECV_SLOTS)].astype(F32)).astype(BF16)

                @pl.when((k < n_ev - RECV_SLOTS) | (layer == 0))
                def _():
                    pl.semaphore_signal(r.credit, inc=1, device_id={'tp': middle}, device_id_type=MESH)

            @pl.when((k >= 2) & (k <= n_ev))
            def _():
                with jax.named_scope('w3'):
                    hop3(k - 2).wait_send()

            @pl.when(k == n_ev)
            def _():
                hop3(n_ev - 1).wait_send()

        @pl.when(outer & (m >= 0))
        def _():
            with jax.named_scope('wo'):
                hop1(m).wait_send()
                hop3(m).wait_recv()
        late = jnp.where(inner, k, m)

        @pl.when((late >= 0) & (late < n_ev))
        def _():
            with jax.named_scope('norm'):
                normalize(layer, late)

            @pl.when(inner)
            def _():
                hop3(late).start()
        piece = n - 14

        @pl.when((layer == 0) & (piece >= 0) & (piece < per_shard * 2))
        def _():
            i = piece // 2

            @pl.when(lax.rem(piece, 2) == 0)
            def _():
                c_across(i)[0].wait_recv()
                c_relay(i)[0].start()

            @pl.when(lax.rem(piece, 2) == 1)
            def _():
                c_across(i)[1].wait_recv()
                c_relay(i)[1].start()

    def event_loop(low, high):
        def body(clock, carry):
            event(clock)
            return carry
        lax.fori_loop(low, high, body, 0)

    def project_chunk(layer, c):
        these = chunk_rows(c)

        def tile(t, carry):
            first = c * n_dim + t * O_TILES
            for i in range(O_TILES):
                wo_copy(layer, first + i).wait()
            for i in range(O_TILES):
                part[these, cols(t * O_TILES + i)] = dot(qo[these, :], wo_place(first + i)[0][...]).astype(BF16)
            for i in range(O_TILES):
                @pl.when(first + i + places < N_CHUNK * n_dim)
                def _():
                    wo_copy(layer, first + i + places).start()
            return carry
        lax.fori_loop(0, n_dim // O_TILES, tile, 0)
        send_chunk(c * N_SUB)

    @pl.when(is_first)
    def _():
        for copy in old_copies:
            copy.wait()
    span = rows + chunk

    def window_chunk(c, carry):
        @pl.when(jnp.logical_not(is_first))
        def _():
            for copy in window_sends(c):
                copy.wait_recv()
        these = chunk_rows(c)
        seen_keys = pl.ds(pl.multiple_of(row_start(c), chunk), span)
        row_id = lax.broadcasted_iota(jnp.int32, (chunk, span), 0)
        col_id = lax.broadcasted_iota(jnp.int32, (chunk, span), 1)
        seen = (col_id > row_id) & (col_id <= row_id + rows)
        def one_head(n, carry):
            kv = cols(n // groups)
            scores = jnp.where(seen, dot_t(qo[these, cols(n)], keys[seen_keys, kv]), NEG_BIG)
            best = jnp.max(scores, axis=-1, keepdims=True)
            prob = jnp.exp(scores - best)
            total = jnp.sum(prob, axis=-1, keepdims=True)
            qo[these, cols(n)] = (dot(prob.astype(BF16), values[seen_keys, kv]) / total).astype(BF16)
            return carry
        lax.fori_loop(0, n_q, one_head, 0)
        with jax.named_scope('proj'):
            project_chunk(0, c)

        @pl.when(c > 0)
        def _():
            event(c - 1)
        return carry
    lax.fori_loop(0, N_CHUNK, window_chunk, 0)
    start_gu(0)

    @pl.when(jnp.logical_not(is_last))
    def _():
        for c in range(N_CHUNK):
            for copy in window_sends(c):
                copy.wait_send()
    for copy in kv_out:
        copy.wait()

    def feed_forward(layer, clock):
        marks = spread(N_SUB, [2] * n_ff + [1] * n_dim)

        def ffn_chunk(c, carry):
            these = chunk_rows(c)

            def task(t, carry):
                @pl.when(t < n_ff)
                def _():
                    i = c * n_ff + t
                    with jax.named_scope('wgu'):
                        for copy in gu_copies(layer, i):
                            copy.wait()
                    slot = lax.rem(i, W_SLOTS // 2) * 2
                    lhs = part[these, :]
                    gate = dot(lhs, wt[slot])
                    up = dot(lhs, wt[slot + 1])
                    hact[:, cols(t)] = (jax.nn.gelu(gate, approximate=True) * up).astype(BF16)

                    @pl.when(i + W_SLOTS // 2 < N_CHUNK * n_ff)
                    def _():
                        for copy in gu_copies(layer, i + W_SLOTS // 2):
                            copy.start()

                @pl.when(t >= n_ff)
                def _():
                    i = c * n_dim + t - n_ff
                    with jax.named_scope('wdn'):
                        dn_copy(layer, i).wait()
                    part[these, cols(t - n_ff)] = dot(hact[...], dn[lax.rem(i, D_SLOTS)]).astype(BF16)

                    @pl.when(i + D_SLOTS < N_CHUNK * n_dim)
                    def _():
                        dn_copy(layer, i + D_SLOTS).start()
                hit = t == marks[0]
                which = jnp.int32(0)
                for mark in marks[1:]:
                    which = which + (t >= mark).astype(jnp.int32)
                    hit = hit | (t == mark)

                @pl.when(hit)
                def _():
                    event(clock + c * N_SUB + which)
                return carry
            with jax.named_scope('ffn'):
                lax.fori_loop(0, n_ff + n_dim, task, 0)
            send_chunk(per + c * N_SUB)
            return carry
        lax.fori_loop(0, N_CHUNK, ffn_chunk, 0)
    lead = N_SUB + LAG
    event_loop(N_CHUNK - 1, lead)
    feed_forward(0, lead)
    start_dn(1)

    def turn_copies(c):
        return [pltpu.make_async_copy(table.at[chunk_rows(c)], r.turn.at[i], r.t_sem.at[i]) for i, table in enumerate((r.cos_global, r.sin_global))]

    def start_project(c):
        for copy in turn_copies(c):
            copy.start()
        for j in range(W_SLOTS):
            start_w(1, jnp.int32(j))
    start_project(0)

    new_names = ((r.k_all_1, r.k_new_1), (r.v_all_1, r.v_new_1))

    def new_sends(c):
        buf = lax.rem(c, 2)
        return [to_cp(r.fresh.at[buf, i], dst.at[cp, chunk_rows(c)], (r.n_s, r.n_r), c * 6 + 2 * k + i, peer) for k, peer in enumerate((across, far, near)) for i, (dst, _) in enumerate(new_names)]

    def new_local(c):
        buf = lax.rem(c, 2)
        return [pltpu.make_async_copy(r.fresh.at[buf, i], place, r.own_sem.at[buf, 2 * i + k]) for i, (every, mine) in enumerate(new_names) for k, place in enumerate((every.at[cp, chunk_rows(c)], mine.at[chunk_rows(c)]))]

    def free_fresh(c):
        for copy in new_sends(c):
            copy.wait_send()
        for copy in new_local(c):
            copy.wait()

    def global_project(c):
        these = chunk_rows(c)
        buf = lax.rem(c, 2)
        @pl.when(c >= 2)
        def _():
            free_fresh(c - 2)
        for copy in turn_copies(c):
            copy.wait()

        def tile(j):
            wait_w(1, j)
            return dot(part[these, :], wt[lax.rem(j, W_SLOTS)])

        def gv_step(j, carry):
            r.fresh[buf, 1, :, cols(j)] = tile(j).astype(BF16)
            start_w(1, j + W_SLOTS)
            return carry

        def gk_step(j, carry):
            r.fresh[buf, 0, :, cols(j)] = rope(tile(j + n_kv), r.turn[0], r.turn[1], 1.0 + qk_ref[3:4, :]).astype(BF16)
            start_w(1, j + n_kv + W_SLOTS)
            return carry

        def gq_step(j, carry):
            qo[these, cols(j)] = as_query(rope(tile(j + 2 * n_kv), r.turn[0], r.turn[1], 1.0 + qk_ref[2:3, :]))
            start_w(1, j + 2 * n_kv + W_SLOTS)
            return carry
        lax.fori_loop(0, n_kv, gv_step, 0)
        lax.fori_loop(0, n_kv, gk_step, 0)
        for copy in new_sends(c) + new_local(c):
            copy.start()
        lax.fori_loop(0, n_q, gq_step, 0)

        @pl.when(c + 1 < N_CHUNK)
        def _():
            start_project(c + 1)

    n_pass = 2 * per_shard
    n_mask = -(-(shard // 2) // block)
    first_pos = r.first_pos[0]
    stack = groups * chunk
    step = min(256, stack)
    scores_refs = (r.s_even, r.s_odd)
    pair = cp // 2

    def pass_size(p):
        return jnp.where(p == 2, cp + 1, n_pass)

    def shard_of(p, b):
        return 2 * lax.rem(pair + p, 2) + lax.rem(b // per_shard, 2)

    def fetch(p, b, own, every, new, dst, sem):
        s = shard_of(p, b)
        where = aligned(lax.rem(b, per_shard) * block, block)

        @pl.when((p < 2) & (s == cp))
        def _():
            pltpu.make_async_copy(own.at[where], dst, sem).start()

        @pl.when((p < 2) & (s != cp))
        def _():
            pltpu.make_async_copy(every.at[s, where], dst, sem).start()

        @pl.when(p == 2)
        def _():
            pltpu.make_async_copy(new.at[lax.rem(b, size)], dst, sem).start()

    def fetch_k(p, b):
        slot = lax.rem(b, 3)
        fetch(p, b, r.k_own, r.k_all, r.k_all_1, keys.at[aligned(slot * block, block)], r.kb_sem.at[slot])

    def fetch_v(p, b):
        slot = lax.rem(b, 2)
        fetch(p, b, r.v_own, r.v_all, r.v_all_1, values.at[aligned(slot * block, block)], r.vb_sem.at[slot])

    def have_k(b):
        slot = lax.rem(b, 3)
        pltpu.make_async_copy(r.k_all_1.at[0], keys.at[aligned(slot * block, block)], r.kb_sem.at[slot]).wait()

    def have_v(b):
        slot = lax.rem(b, 2)
        pltpu.make_async_copy(r.v_all_1.at[0], values.at[aligned(slot * block, block)], r.vb_sem.at[slot]).wait()

    def begin_pass(p):
        fetch_k(p, 0)
        fetch_v(p, 0)

        @pl.when(pass_size(p) > 1)
        def _():
            fetch_k(p, 1)

    def raw_scores(c, head, slot):
        query = jnp.concatenate([qo[chunk_rows(c), (head * groups + g) * HEAD:(head * groups + g + 1) * HEAD] for g in range(groups)], axis=0)
        scores_refs[head][...] = dot_t(query, keys[aligned(slot * block, block), head * HEAD:(head + 1) * HEAD])

    def state(c, head, low, length):
        return aligned(lax.rem(c, 2) * half + head * stack + low, length)

    def absorb(c, head, slot, bound):
        value = values[aligned(slot * block, block), head * HEAD:(head + 1) * HEAD]
        for low in range(0, stack, step):
            scores = scores_refs[head][low:low + step, :]
            if bound is not None:
                limit, by_row = bound
                row_id = lax.rem(low, chunk) + lax.rem(lax.broadcasted_iota(jnp.int32, scores.shape, 0), chunk)
                scores = jnp.where(lax.broadcasted_iota(jnp.int32, scores.shape, 1) < limit + by_row * row_id, scores, NEG_BIG)
            these = state(c, head, low, step)
            old = top[these, :]
            new = jnp.maximum(old, jnp.max(scores, axis=-1, keepdims=True))
            decay = jnp.exp(old - new)
            prob = jnp.exp(scores - jnp.concatenate([new] * (block // 128), axis=1))
            lanes = prob[:, :128]
            for i in range(1, block // 128):
                lanes = lanes + prob[:, i * 128:(i + 1) * 128]
            sums[these, :] = sums[these, :] * decay + lanes
            top[these, :] = new
            acc_ref[these, :] = acc_ref[these, :] * jnp.concatenate([decay] * (HEAD // 128), axis=1) + dot(prob.astype(BF16), value)

    def job_step(j, carry):
        second = j // 6
        c = (1 - second) * lax.rem(j, 2) + second * (j // 3)
        p = (1 - second) * (j // 2) + second * lax.rem(j, 3)

        @pl.when((j < 2) | (j == 3))
        def _():
            low = j - j // 3

            def body(i, carry):
                before = lead + 16 + 3 * i + 2 * (i // 2) - 2 * (i // 3)
                event_loop(before, before + 1 + 2 * (i // 3))
                with jax.named_scope('qkv1'):
                    global_project(i)
                return carry
            lax.fori_loop(low, low + 1 + j // 3, body, 0)

            @pl.when(j == 3)
            def _():
                start_wo(1)

        @pl.when(p == 0)
        def _():
            for ref, value in ((top, NEG_BIG), (sums, 0.0), (acc_ref, 0.0)):
                ref[state(c, 0, 0, half), :] = jnp.full((half, ref.shape[1]), value, F32)
        count = pass_size(p)
        n_free = jnp.where(p == 2, cp, n_pass - n_mask)
        base = jnp.where(second == 1, n_tick + 1 + 5 * ((j - 6) // 3) + 2 * lax.rem(j, 3), jnp.where(j == 5, n_tick, lead + 17 + 3 * j - j // 2))
        have_k(0)
        raw_scores(c, 0, 0)

        def block_step(masked, b, carry):
            have_v(b)

            @pl.when(b + 1 < count)
            def _():
                have_k(b + 1)
                fetch_v(p, b + 1)

            @pl.when(b + 2 < count)
            def _():
                fetch_k(p, b + 2)
            bound = None
            if masked:
                limit = jnp.where(p == 2, row_start(c) + 1, jnp.where(shard_of(p, b) == size - 1, first_pos - (size - 1) * shard - lax.rem(b, per_shard) * block, block))
                bound = (limit, jnp.where(p == 2, 1, 0))
            slot, later, v_slot = lax.rem(b, 3), lax.rem(b + 1, 3), lax.rem(b, 2)
            raw_scores(c, 1, slot)
            absorb(c, 0, v_slot, bound)
            raw_scores(c, 0, later)
            absorb(c, 1, v_slot, bound)
            if not masked:
                @pl.when((b == (n_pass - n_mask) // 2) & (p < 2) & (j != 3))
                def _():
                    event(base)
            return carry
        with jax.named_scope('blocks'):
            lax.fori_loop(0, n_free, functools.partial(block_step, False), 0)
            lax.fori_loop(n_free, count, functools.partial(block_step, True), 0)

        @pl.when(j == 1)
        def _():
            def body(i, carry):
                with jax.named_scope('wrly'):
                    for copy in c_relay(i):
                        copy.wait_recv()
                return carry
            lax.fori_loop(0, per_shard, body, 0)

        @pl.when(j == 3)
        def _():
            free_fresh(2)
            free_fresh(3)

            def body(i, carry):
                with jax.named_scope('wnew'):
                    for copy in new_sends(i):
                        copy.wait_recv()
                return carry
            lax.fori_loop(0, N_CHUNK, body, 0)

        @pl.when(j < 11)
        def _():
            after = j + 1
            begin_pass((1 - after // 6) * (after // 2) + (after // 6) * lax.rem(after, 3))

        @pl.when(p == 2)
        def _():
            these = chunk_rows(c)
            for head in range(n_kv):
                whole = state(c, head, 0, stack)
                total = jnp.sum(sums[whole, :], axis=-1, keepdims=True)
                result = (acc_ref[whole, :] / total).astype(BF16)
                for g in range(groups):
                    qo[these, (head * groups + g) * HEAD:(head * groups + g + 1) * HEAD] = result[g * chunk:(g + 1) * chunk]
            with jax.named_scope('proj'):
                project_chunk(1, c)

        @pl.when((j != 3) & (j != 4))
        def _():
            event(base + jnp.where(p < 2, 1, 0))
        return carry
    for copy in c_near:
        copy.wait()
    begin_pass(jnp.int32(0))
    lax.fori_loop(0, 12, job_step, 0)
    start_gu(1)
    clock = n_tick + 11
    feed_forward(1, clock)
    event_loop(clock + N_CHUNK * N_SUB, 2 * n_tick)

    def finish(m, carry):
        out_copy(m).wait()
        return carry
    lax.fori_loop(0, per, finish, 0)

    def gathered(i, carry):
        for copy in c_across(i) + c_relay(i):
            copy.wait_send()
        return carry
    lax.fori_loop(0, per_shard, gathered, 0)


def run_layers(ins, collective_id):
    rows, dim = ins['x'].shape
    q_cols, kv_cols, ff = ins['w_query'].shape[2], ins['w_key'].shape[2], ins['w_gate'].shape[2]
    shard = ins['k_own'].shape[0]
    chunk = rows // N_CHUNK
    sub = chunk // N_SUB
    n_ev = 2 * N_CHUNK * N_SUB
    groups, n_kv = q_cols // kv_cols, kv_cols // HEAD
    stack = groups * chunk
    pieces = 2 * (shard // rows)

    def spec(name):
        if name == 'first_pos':
            return pl.BlockSpec(memory_space=pltpu.SMEM)
        return pl.BlockSpec(memory_space=pltpu.VMEM if name in ('gains', 'qk_gains') else pl.ANY)
    array = jax.ShapeDtypeStruct
    made = array((rows, kv_cols), BF16)
    outs = dict(x_out=array((rows, dim), BF16), k_new_0=made, v_new_0=made, k_new_1=made, v_new_1=made)
    outs |= dict(k_all=array((4, shard, kv_cols), BF16), v_all=array((4, shard, kv_cols), BF16), k_all_1=array((4, rows, kv_cols), BF16), v_all_1=array((4, rows, kv_cols), BF16))
    dma = pltpu.SemaphoreType.DMA
    scratch = dict(
        part=pltpu.VMEM((rows, dim), BF16),
        tot=pltpu.VMEM((rows, dim), BF16),
        xv=pltpu.VMEM((rows, dim), BF16),
        wt=pltpu.VMEM((W_SLOTS, dim, TILE), BF16),
        dn=pltpu.VMEM((D_SLOTS, ff, TILE), BF16),
        qo=pltpu.VMEM((rows, q_cols), BF16),
        hact=pltpu.VMEM((chunk, ff), BF16),
        recv2=pltpu.VMEM((RECV_SLOTS, sub, dim), BF16),
        keys=pltpu.VMEM((3 * rows, kv_cols), BF16),
        values=pltpu.VMEM((2 * rows, kv_cols), BF16),
        fresh=pltpu.VMEM((2, 2, chunk, kv_cols), BF16),
        turn=pltpu.VMEM((2, chunk, HEAD // 2), F32),
        s_even=pltpu.VMEM((stack, rows), F32),
        s_odd=pltpu.VMEM((stack, rows), F32),
        top=pltpu.VMEM((2 * n_kv * stack, 128), F32),
        sums=pltpu.VMEM((2 * n_kv * stack, 128), F32),
        acc=pltpu.VMEM((2 * n_kv * stack, HEAD), F32),
        w_sem=dma((W_SLOTS,)), wo_sem=dma((W_SLOTS * (dim // q_cols),)), dn_sem=dma((D_SLOTS,)), x_sem=dma((N_CHUNK,)), t_sem=dma((2,)), old_sem=dma((2,)),
        kv_sem=dma((2,)), own_sem=dma((2, 4)), kb_sem=dma((3,)), vb_sem=dma((2,)), out_sem=dma((n_ev // 2,)),
        w_s=dma((2 * N_CHUNK,)), w_r=dma((2 * N_CHUNK,)), n_s=dma((6 * N_CHUNK,)), n_r=dma((6 * N_CHUNK,)),
        c_near_s=dma((2,)), c_near_r=dma((2,)), c_across_s=dma((pieces,)), c_across_r=dma((pieces,)), c_relay_s=dma((pieces,)), c_relay_r=dma((pieces,)),
        s1=dma((n_ev,)), s2s=dma((n_ev,)), s2r=dma((n_ev,)), s3=dma((n_ev,)),
        credit=pltpu.SemaphoreType.REGULAR,
    )
    names = tuple(ins) + tuple(outs) + tuple(scratch)
    made = pl.pallas_call(
        functools.partial(layers_kernel, names),
        out_shape=tuple(outs.values()),
        in_specs=[spec(name) for name in ins],
        out_specs=tuple(pl.BlockSpec(memory_space=pl.ANY) for _ in outs),
        scratch_shapes=list(scratch.values()),
        compiler_params=pltpu.CompilerParams(collective_id=collective_id, has_side_effects=True, vmem_limit_bytes=VMEM_LIMIT),
        name='two_layers',
    )(*ins.values())
    return dict(zip(outs, made))


def leave_kernel(n_kv, *refs):
    half = len(refs) // 2
    refs[half][...] = refs[0][...]
    for flat, shaped in zip(refs[1:half], refs[half + 1:]):
        for head in range(n_kv):
            shaped[:, head, :] = flat[:, head * HEAD:(head + 1) * HEAD]


def leave(x, *flats):
    rows, dim = x.shape
    kv_cols = flats[0].shape[1]
    n_kv, step = kv_cols // HEAD, rows // 8
    wide = pl.BlockSpec((step, dim), lambda i: (i, 0))
    flat = pl.BlockSpec((step, kv_cols), lambda i: (i, 0))
    shaped = pl.BlockSpec((step, n_kv, HEAD), lambda i: (i, 0, 0))
    return pl.pallas_call(
        functools.partial(leave_kernel, n_kv),
        grid=(8,),
        out_shape=(jax.ShapeDtypeStruct((rows, dim), BF16),) + (jax.ShapeDtypeStruct((rows, n_kv, HEAD), BF16),) * len(flats),
        in_specs=[wide] + [flat] * len(flats),
        out_specs=(wide,) + (shaped,) * len(flats),
        name='leave',
    )(x, *flats)


def solution(mesh):
    row_spec = P(('dp', 'cp'), None)
    cache_spec = P(('dp', 'cp'), 'tp', None)
    window_spec = P('dp', 'tp', None)
    col_spec = P(None, None, 'tp')
    row_split = P(None, 'tp', None)
    replicated = P()

    def device_step(hidden, start_pos, k_local, v_local, k_global, v_global, w_query, w_key, w_value, w_out, w_gate, w_up, w_down, norm_gain, qk_gain):
        first_pos = start_pos[0]
        cp_index = lax.axis_index('cp')
        rows, dim = hidden.shape
        window = k_local.shape[0]
        flat = lambda a: a.reshape(a.shape[0], -1)
        gains = jnp.concatenate([norm_gain.reshape(8, dim), jnp.zeros((8, dim), F32)], axis=0)
        qk_gains = jnp.concatenate([qk_gain.reshape(4, HEAD), jnp.zeros((4, HEAD), F32)], axis=0)
        turn = jnp.remainder(first_pos, window)
        rolled = [flat(lax.dynamic_slice_in_dim(jnp.concatenate([a, a], axis=0), turn, window, axis=0)) for a in (k_local, v_local)]
        cos_local, sin_local = rope_tables(first_pos + cp_index * rows, rows, LOCAL_BASE, 1.0)
        cos_global, sin_global = rope_tables(first_pos + cp_index * rows, rows, GLOBAL_BASE, GLOBAL_DIV)
        made = run_layers(dict(
            first_pos=start_pos, x=hidden, gains=gains, qk_gains=qk_gains,
            cos_local=cos_local, sin_local=sin_local, cos_global=cos_global, sin_global=sin_global,
            w_query=w_query, w_key=w_key, w_value=w_value, w_out=w_out, w_gate=w_gate, w_up=w_up, w_down=w_down,
            k_old=rolled[0], v_old=rolled[1], k_own=flat(k_global), v_own=flat(v_global),
        ), 0)
        return leave(made['x_out'], made['k_new_0'], made['v_new_0'], made['k_new_1'], made['v_new_1'])

    return jax.shard_map(device_step, mesh=mesh, in_specs=(row_spec, P('dp'), window_spec, window_spec, cache_spec, cache_spec, col_spec, col_spec, col_spec, row_split, col_spec, col_spec, row_split, replicated, replicated), out_specs=(row_spec, cache_spec, cache_spec, cache_spec, cache_spec), check_vma=False)
```

```python
import functools
import types

import jax
import jax.numpy as jnp
from jax import lax
from jax.experimental import pallas as pl
from jax.experimental.pallas import tpu as pltpu
from jax.sharding import PartitionSpec as P

NORM_EPS = 1e-6
LOCAL_BASE = 10000.0
GLOBAL_BASE = 1000000.0
GLOBAL_DIV = 8.0
NEG_BIG = -1e30
HEAD = 256
TILE = 256
VMEM_LIMIT = 67_000_000
MESH = pl.DeviceIdType.MESH
F32 = jnp.float32
BF16 = jnp.bfloat16


def dot(a, b):
    return jnp.dot(a, b, preferred_element_type=F32)


def dot_t(a, b):
    return lax.dot_general(a, b, (((1,), (1,)), ((), ())), preferred_element_type=F32)


def unit_rms(values):
    return values * lax.rsqrt(jnp.mean(values * values, axis=-1, keepdims=True) + NORM_EPS)


def rope_tables(first, rows, rope_base, divisor):
    half, step = HEAD // 2, 32
    inv_freq = 1.0 / (rope_base ** (jnp.arange(0, 2 * half, 2, dtype=F32) / (2 * half)))
    fine = (jnp.arange(step).astype(F32) / divisor)[:, None] * inv_freq[None, :]
    coarse = ((first + jnp.arange(0, rows, step)).astype(F32) / divisor)[:, None] * inv_freq[None, :]
    cos_f, sin_f, cos_c, sin_c = lax.optimization_barrier((jnp.cos(fine)[None], jnp.sin(fine)[None], jnp.cos(coarse)[:, None], jnp.sin(coarse)[:, None]))
    return (cos_c * cos_f - sin_c * sin_f).reshape(rows, half), (sin_c * cos_f + cos_c * sin_f).reshape(rows, half)


def enter(peers):
    for peer in peers:
        pl.semaphore_signal(pltpu.get_barrier_semaphore(), inc=1, device_id=peer, device_id_type=MESH)


def entered(peers):
    pl.semaphore_wait(pltpu.get_barrier_semaphore(), len(peers))


N_CHUNK = 4
N_SUB = 4
RECV_SLOTS = 3
LAG = 2
W_SLOTS = 6
D_SLOTS = 3
O_TILES = 3


def spread(count, weights):
    total, seen, marks = sum(weights), 0, []
    for i, weight in enumerate(weights):
        seen += weight
        if seen * count >= total * (len(marks) + 1):
            marks.append(i)
    return marks


def layers_kernel(names, *refs):
    r = types.SimpleNamespace(**dict(zip(names, refs)))
    x_hbm, g_ref, qk_ref = r.x, r.gains, r.qk_gains
    part, tot, xv, wt, dn, qo, hact, recv2 = r.part, r.tot, r.xv, r.wt, r.dn, r.qo, r.hact, r.recv2
    keys, values, top, sums, acc_ref = r.keys, r.values, r.top, r.sums, r.acc
    rows, dim = x_hbm.shape
    ff = r.w_gate.shape[2]
    kv_cols = r.w_key.shape[2]
    q_cols = r.w_query.shape[2]
    n_kv, n_q = kv_cols // HEAD, q_cols // HEAD
    groups = n_q // n_kv
    chunk = rows // N_CHUNK
    sub = chunk // N_SUB
    per = N_CHUNK * N_SUB
    n_ev = 2 * per
    n_tick = n_ev + LAG
    n_dim, n_ff = dim // TILE, ff // TILE
    tp, cp, size = lax.axis_index('tp'), lax.axis_index('cp'), lax.axis_size('cp')
    outer = (tp == 0) | (tp == 3)
    inner = jnp.logical_not(outer)
    mate = tp + 1 - 2 * lax.rem(tp, 2)
    middle = 3 - tp
    near = cp + 1 - 2 * lax.rem(cp, 2)
    across = lax.rem(cp + 2, size)
    far = lax.rem(near + 2, size)
    right = lax.rem(cp + 1, size)
    is_first, is_last = cp == 0, cp == size - 1

    def aligned(start, length):
        return pl.ds(pl.multiple_of(start, length), length)

    def cols(t):
        return aligned(t * TILE, TILE)

    def row_start(c):
        return (N_CHUNK - 1 - c) * chunk

    def chunk_rows(c):
        return aligned(row_start(c), chunk)

    def sub_start(n):
        m = lax.rem(n, per)
        return row_start(m // N_SUB) + lax.rem(m, N_SUB) * sub

    def rows_of(n):
        return aligned(sub_start(n), sub)

    n_tile = 2 * n_kv + n_q

    def start_w(layer, j):
        for low, high, w_hbm in ((0, n_kv, r.w_value), (n_kv, 2 * n_kv, r.w_key), (2 * n_kv, n_tile, r.w_query)):
            @pl.when((j >= low) & (j < high))
            def _():
                slot = lax.rem(j, W_SLOTS)
                pltpu.make_async_copy(w_hbm.at[layer, :, cols(jnp.clip(j - low, 0, high - low - 1))], wt.at[slot], r.w_sem.at[slot]).start()

    def wait_w(layer, j):
        slot = lax.rem(j, W_SLOTS)
        pltpu.make_async_copy(r.w_value.at[layer, :, cols(0)], wt.at[slot], r.w_sem.at[slot]).wait()

    per_slot = dim // q_cols
    places = W_SLOTS * per_slot

    def wo_place(k):
        place = lax.rem(k, places)
        return wt.at[place // per_slot, aligned(lax.rem(place, per_slot) * q_cols, q_cols)], r.wo_sem.at[place]

    def wo_copy(layer, k):
        dst, sem = wo_place(k)
        return pltpu.make_async_copy(r.w_out.at[layer, :, cols(lax.rem(k, n_dim))], dst, sem)

    def start_wo(layer):
        def body(k, carry):
            wo_copy(layer, k).start()
            return carry
        lax.fori_loop(0, places, body, 0)

    def gu_copies(layer, i):
        slot, t = lax.rem(i, W_SLOTS // 2) * 2, lax.rem(i, n_ff)
        return [pltpu.make_async_copy(w.at[layer, :, cols(t)], wt.at[slot + k], r.w_sem.at[slot + k]) for k, w in enumerate((r.w_gate, r.w_up))]

    def dn_copy(layer, i):
        slot = lax.rem(i, D_SLOTS)
        return pltpu.make_async_copy(r.w_down.at[layer, :, cols(lax.rem(i, n_dim))], dn.at[slot], r.dn_sem.at[slot])

    def start_gu(layer):
        for i in range(W_SLOTS // 2):
            for copy in gu_copies(layer, jnp.int32(i)):
                copy.start()

    def start_dn(layer):
        for i in range(D_SLOTS):
            dn_copy(layer, jnp.int32(i)).start()

    peers = [{'tp': mate}, {'tp': middle}, {'cp': near}, {'cp': across}, {'cp': far}]
    enter(peers)
    x_copies = [pltpu.make_async_copy(x_hbm.at[pl.ds(i * chunk, chunk)], xv.at[pl.ds(i * chunk, chunk)], r.x_sem.at[i]) for i in range(N_CHUNK)]
    x_copies[0].start()
    start_w(0, jnp.int32(0))
    for copy in x_copies[1:]:
        copy.start()
    for j in range(1, W_SLOTS):
        start_w(0, jnp.int32(j))
    half = n_kv * groups * chunk
    cos_ref, sin_ref = top.at[pl.ds(0, half)], sums.at[pl.ds(0, half)]
    t_copies = [pltpu.make_async_copy(table, dst, r.t_sem.at[i]) for i, (table, dst) in enumerate(((r.cos_local, cos_ref), (r.sin_local, sin_ref)))]
    for copy in t_copies:
        copy.start()
    start_dn(0)
    old_copies = [pltpu.make_async_copy(old, buf.at[pl.ds(0, rows)], r.old_sem.at[i]) for i, (old, buf) in enumerate(((r.k_old, keys), (r.v_old, values)))]

    @pl.when(is_first)
    def _():
        for copy in old_copies:
            copy.start()

    def to_cp(src, dst, sems, i, peer):
        return pltpu.make_async_remote_copy(src_ref=src, dst_ref=dst, send_sem=sems[0].at[i], recv_sem=sems[1].at[i], device_id={'cp': peer}, device_id_type=MESH)

    block = rows
    shard = r.k_own.shape[0]
    per_shard = shard // block
    own_names = ((r.k_own, r.k_all), (r.v_own, r.v_all))
    c_near = [to_cp(src, dst.at[cp], (r.c_near_s, r.c_near_r), i, near) for i, (src, dst) in enumerate(own_names)]

    def c_across(i):
        where = aligned(i * block, block)
        return [to_cp(src.at[where], dst.at[cp, where], (r.c_across_s, r.c_across_r), 2 * i + k, across) for k, (src, dst) in enumerate(own_names)]

    def c_relay(i):
        where = aligned(i * block, block)
        return [to_cp(dst.at[across, where], dst.at[across, where], (r.c_relay_s, r.c_relay_r), 2 * i + k, near) for k, (src, dst) in enumerate(own_names)]
    def rope(acc, cos, sin, gain):
        scaled = unit_rms(acc) * gain
        low, high = scaled[:, :HEAD // 2], scaled[:, HEAD // 2:]
        return jnp.concatenate([low * cos - high * sin, high * cos + low * sin], axis=-1)

    def as_query(value):
        return (value.astype(BF16).astype(F32) * (HEAD ** -0.5)).astype(BF16)

    for i in range(N_CHUNK):
        x_copies[i].wait()

        def norm_rows(k, carry):
            these = aligned(i * chunk + k * 32, 32)
            part[these, :] = (unit_rms(xv[these, :].astype(F32)) * (1.0 + g_ref[0:1, :])).astype(BF16)
            return carry
        lax.fori_loop(0, chunk // 32, norm_rows, 0)
    for copy in t_copies:
        copy.wait()

    tall = 2 * chunk

    def local_tile(j, put):
        wait_w(0, j)

        def rows_step(c, carry):
            these = aligned(c * tall, tall)
            put(c, these, dot(part[these, :], wt[lax.rem(j, W_SLOTS)]))
            return carry
        lax.fori_loop(0, rows // tall, rows_step, 0)
        start_w(0, j + W_SLOTS)

    def v_step(j, carry):
        def put(c, these, acc):
            values[aligned(rows + c * tall, tall), cols(j)] = acc.astype(BF16)
        local_tile(j, put)
        return carry

    def k_step(j, carry):
        def put(c, these, acc):
            keys[aligned(rows + c * tall, tall), cols(j)] = rope(acc, cos_ref[these, :], sin_ref[these, :], 1.0 + qk_ref[1:2, :]).astype(BF16)
        local_tile(j + n_kv, put)
        return carry

    def q_step(j, carry):
        def put(c, these, acc):
            qo[these, cols(j)] = as_query(rope(acc, cos_ref[these, :], sin_ref[these, :], 1.0 + qk_ref[0:1, :]))
        local_tile(j + 2 * n_kv, put)
        return carry
    lax.fori_loop(0, n_kv, v_step, 0)
    lax.fori_loop(0, n_kv, k_step, 0)

    def window_sends(c):
        return [to_cp(buf.at[aligned(rows + row_start(c), chunk)], buf.at[chunk_rows(c)], (r.w_s, r.w_r), 2 * c + i, right) for i, buf in enumerate((keys, values))]

    entered(peers)

    @pl.when(jnp.logical_not(is_last))
    def _():
        for c in range(N_CHUNK):
            for copy in window_sends(c):
                copy.start()
    for copy in c_near:
        copy.start()

    def across_start(i, carry):
        for copy in c_across(i):
            copy.start()
        return carry
    lax.fori_loop(0, per_shard, across_start, 0)
    kv_out = [pltpu.make_async_copy(buf.at[pl.ds(rows, rows)], dst, r.kv_sem.at[i]) for i, (buf, dst) in enumerate(((keys, r.k_new_0), (values, r.v_new_0)))]
    for copy in kv_out:
        copy.start()
    lax.fori_loop(0, n_q, q_step, 0)
    start_wo(0)

    def to_tp(src, dst, send_sem, recv_sem, peer):
        return pltpu.make_async_remote_copy(src_ref=src, dst_ref=dst, send_sem=send_sem, recv_sem=recv_sem, device_id={'tp': peer}, device_id_type=MESH)

    def hop1(n):
        return to_tp(part.at[rows_of(n)], tot.at[rows_of(n)], r.s1.at[n], r.s1.at[n], mate)

    def recv_slot(layer, n):
        return lax.rem(layer * n_ev + n, RECV_SLOTS)

    def hop2(layer, n):
        return to_tp(part.at[rows_of(n)], recv2.at[recv_slot(layer, n)], r.s2s.at[n], r.s2r.at[n], middle)

    def hop3(n):
        return to_tp(tot.at[rows_of(n)], tot.at[rows_of(n)], r.s3.at[n], r.s3.at[n], mate)

    def out_copy(n):
        return pltpu.make_async_copy(xv.at[rows_of(n)], r.x_out.at[rows_of(n)], r.out_sem.at[lax.rem(n, per)])

    def send_chunk(first):
        @pl.when(outer)
        def _():
            for i in range(N_SUB):
                hop1(first + i).start()

    def normalize(layer, n):
        start = sub_start(n)
        step = min(32, sub)
        kind = n // per

        def body(i, carry):
            these = aligned(start + i * step, step)
            value = (xv[these, :].astype(F32) + unit_rms(tot[these, :].astype(F32)) * (1.0 + g_ref[pl.ds(4 * layer + 1 + 2 * kind, 1), :])).astype(BF16)
            xv[these, :] = value
            part[these, :] = (unit_rms(value.astype(F32)) * (1.0 + g_ref[pl.ds(4 * layer + 2 + 2 * kind, 1), :])).astype(BF16)
            return carry
        lax.fori_loop(0, sub // step, body, 0)

        @pl.when((layer == 1) & (kind == 1))
        def _():
            out_copy(n).start()

    def event(clock):
        layer = clock // n_tick
        n = lax.rem(clock, n_tick)
        k, m = n - 1, n - LAG

        @pl.when(inner)
        def _():
            @pl.when(n < n_ev)
            def _():
                hop1(n).wait_recv()
                these = rows_of(n)
                part[these, :] = (part[these, :].astype(F32) + tot[these, :].astype(F32)).astype(BF16)

                @pl.when((n >= RECV_SLOTS) | (layer == 1))
                def _():
                    pl.semaphore_wait(r.credit, 1)
                hop2(layer, n).start()

            @pl.when((k >= 0) & (k < n_ev))
            def _():
                hop2(layer, k).wait_recv()
                hop2(layer, k).wait_send()
                these = rows_of(k)
                tot[these, :] = (part[these, :].astype(F32) + recv2[recv_slot(layer, k)].astype(F32)).astype(BF16)

                @pl.when((k < n_ev - RECV_SLOTS) | (layer == 0))
                def _():
                    pl.semaphore_signal(r.credit, inc=1, device_id={'tp': middle}, device_id_type=MESH)

            @pl.when((k >= 2) & (k <= n_ev))
            def _():
                hop3(k - 2).wait_send()

            @pl.when(k == n_ev)
            def _():
                hop3(n_ev - 1).wait_send()

        @pl.when(outer & (m >= 0))
        def _():
            hop1(m).wait_send()
            hop3(m).wait_recv()
        late = jnp.where(inner, k, m)

        @pl.when((late >= 0) & (late < n_ev))
        def _():
            normalize(layer, late)

            @pl.when(inner)
            def _():
                hop3(late).start()
        piece = n - 14

        @pl.when((layer == 0) & (piece >= 0) & (piece < per_shard * 2))
        def _():
            i = piece // 2

            @pl.when(lax.rem(piece, 2) == 0)
            def _():
                c_across(i)[0].wait_recv()
                c_relay(i)[0].start()

            @pl.when(lax.rem(piece, 2) == 1)
            def _():
                c_across(i)[1].wait_recv()
                c_relay(i)[1].start()

    def event_loop(low, high):
        def body(clock, carry):
            event(clock)
            return carry
        lax.fori_loop(low, high, body, 0)

    def project_chunk(layer, c):
        these = chunk_rows(c)

        def tile(t, carry):
            first = c * n_dim + t * O_TILES
            for i in range(O_TILES):
                wo_copy(layer, first + i).wait()
            for i in range(O_TILES):
                part[these, cols(t * O_TILES + i)] = dot(qo[these, :], wo_place(first + i)[0][...]).astype(BF16)
            for i in range(O_TILES):
                @pl.when(first + i + places < N_CHUNK * n_dim)
                def _():
                    wo_copy(layer, first + i + places).start()
            return carry
        lax.fori_loop(0, n_dim // O_TILES, tile, 0)
        send_chunk(c * N_SUB)

    @pl.when(is_first)
    def _():
        for copy in old_copies:
            copy.wait()
    span = rows + chunk

    def window_chunk(c, carry):
        @pl.when(jnp.logical_not(is_first))
        def _():
            for copy in window_sends(c):
                copy.wait_recv()
        these = chunk_rows(c)
        seen_keys = pl.ds(pl.multiple_of(row_start(c), chunk), span)
        row_id = lax.broadcasted_iota(jnp.int32, (chunk, span), 0)
        col_id = lax.broadcasted_iota(jnp.int32, (chunk, span), 1)
        seen = (col_id > row_id) & (col_id <= row_id + rows)
        def one_head(n, carry):
            kv = cols(n // groups)
            scores = jnp.where(seen, dot_t(qo[these, cols(n)], keys[seen_keys, kv]), NEG_BIG)
            best = jnp.max(scores, axis=-1, keepdims=True)
            prob = jnp.exp(scores - best)
            total = jnp.sum(prob, axis=-1, keepdims=True)
            qo[these, cols(n)] = (dot(prob.astype(BF16), values[seen_keys, kv]) / total).astype(BF16)
            return carry
        lax.fori_loop(0, n_q, one_head, 0)
        project_chunk(0, c)

        @pl.when(c > 0)
        def _():
            event(c - 1)
        return carry
    lax.fori_loop(0, N_CHUNK, window_chunk, 0)
    start_gu(0)

    @pl.when(jnp.logical_not(is_last))
    def _():
        for c in range(N_CHUNK):
            for copy in window_sends(c):
                copy.wait_send()
    for copy in kv_out:
        copy.wait()

    def feed_forward(layer, clock):
        marks = spread(N_SUB, [2] * n_ff + [1] * n_dim)

        def ffn_chunk(c, carry):
            these = chunk_rows(c)

            def task(t, carry):
                @pl.when(t < n_ff)
                def _():
                    i = c * n_ff + t
                    for copy in gu_copies(layer, i):
                        copy.wait()
                    slot = lax.rem(i, W_SLOTS // 2) * 2
                    lhs = part[these, :]
                    gate = dot(lhs, wt[slot])
                    up = dot(lhs, wt[slot + 1])
                    hact[:, cols(t)] = (jax.nn.gelu(gate, approximate=True) * up).astype(BF16)

                    @pl.when(i + W_SLOTS // 2 < N_CHUNK * n_ff)
                    def _():
                        for copy in gu_copies(layer, i + W_SLOTS // 2):
                            copy.start()

                @pl.when(t >= n_ff)
                def _():
                    i = c * n_dim + t - n_ff
                    dn_copy(layer, i).wait()
                    part[these, cols(t - n_ff)] = dot(hact[...], dn[lax.rem(i, D_SLOTS)]).astype(BF16)

                    @pl.when(i + D_SLOTS < N_CHUNK * n_dim)
                    def _():
                        dn_copy(layer, i + D_SLOTS).start()
                hit = t == marks[0]
                which = jnp.int32(0)
                for mark in marks[1:]:
                    which = which + (t >= mark).astype(jnp.int32)
                    hit = hit | (t == mark)

                @pl.when(hit)
                def _():
                    event(clock + c * N_SUB + which)
                return carry
            lax.fori_loop(0, n_ff + n_dim, task, 0)
            send_chunk(per + c * N_SUB)
            return carry
        lax.fori_loop(0, N_CHUNK, ffn_chunk, 0)
    lead = N_SUB + LAG
    event_loop(N_CHUNK - 1, lead)
    feed_forward(0, lead)
    start_dn(1)

    def turn_copies(c):
        return [pltpu.make_async_copy(table.at[chunk_rows(c)], r.turn.at[i], r.t_sem.at[i]) for i, table in enumerate((r.cos_global, r.sin_global))]

    def start_project(c):
        for copy in turn_copies(c):
            copy.start()
        for j in range(W_SLOTS):
            start_w(1, jnp.int32(j))
    start_project(0)

    new_names = ((r.k_all_1, r.k_new_1), (r.v_all_1, r.v_new_1))

    def new_sends(c):
        buf = lax.rem(c, 2)
        return [to_cp(r.fresh.at[buf, i], dst.at[cp, chunk_rows(c)], (r.n_s, r.n_r), c * 6 + 2 * k + i, peer) for k, peer in enumerate((across, far, near)) for i, (dst, _) in enumerate(new_names)]

    def new_local(c):
        buf = lax.rem(c, 2)
        return [pltpu.make_async_copy(r.fresh.at[buf, i], place, r.own_sem.at[buf, 2 * i + k]) for i, (every, mine) in enumerate(new_names) for k, place in enumerate((every.at[cp, chunk_rows(c)], mine.at[chunk_rows(c)]))]

    def free_fresh(c):
        for copy in new_sends(c):
            copy.wait_send()
        for copy in new_local(c):
            copy.wait()

    def global_project(c):
        these = chunk_rows(c)
        buf = lax.rem(c, 2)
        @pl.when(c >= 2)
        def _():
            free_fresh(c - 2)
        for copy in turn_copies(c):
            copy.wait()

        def tile(j):
            wait_w(1, j)
            return dot(part[these, :], wt[lax.rem(j, W_SLOTS)])

        def gv_step(j, carry):
            r.fresh[buf, 1, :, cols(j)] = tile(j).astype(BF16)
            start_w(1, j + W_SLOTS)
            return carry

        def gk_step(j, carry):
            r.fresh[buf, 0, :, cols(j)] = rope(tile(j + n_kv), r.turn[0], r.turn[1], 1.0 + qk_ref[3:4, :]).astype(BF16)
            start_w(1, j + n_kv + W_SLOTS)
            return carry

        def gq_step(j, carry):
            qo[these, cols(j)] = as_query(rope(tile(j + 2 * n_kv), r.turn[0], r.turn[1], 1.0 + qk_ref[2:3, :]))
            start_w(1, j + 2 * n_kv + W_SLOTS)
            return carry
        lax.fori_loop(0, n_kv, gv_step, 0)
        lax.fori_loop(0, n_kv, gk_step, 0)
        for copy in new_sends(c) + new_local(c):
            copy.start()
        lax.fori_loop(0, n_q, gq_step, 0)

        @pl.when(c + 1 < N_CHUNK)
        def _():
            start_project(c + 1)

    n_pass = 2 * per_shard
    n_mask = -(-(shard // 2) // block)
    first_pos = r.first_pos[0]
    stack = groups * chunk
    step = min(256, stack)
    scores_refs = (r.s_even, r.s_odd)
    pair = cp // 2

    def pass_size(p):
        return jnp.where(p == 2, cp + 1, n_pass)

    def shard_of(p, b):
        return 2 * lax.rem(pair + p, 2) + lax.rem(b // per_shard, 2)

    def fetch(p, b, own, every, new, dst, sem):
        s = shard_of(p, b)
        where = aligned(lax.rem(b, per_shard) * block, block)

        @pl.when((p < 2) & (s == cp))
        def _():
            pltpu.make_async_copy(own.at[where], dst, sem).start()

        @pl.when((p < 2) & (s != cp))
        def _():
            pltpu.make_async_copy(every.at[s, where], dst, sem).start()

        @pl.when(p == 2)
        def _():
            pltpu.make_async_copy(new.at[lax.rem(b, size)], dst, sem).start()

    def fetch_k(p, b):
        slot = lax.rem(b, 3)
        fetch(p, b, r.k_own, r.k_all, r.k_all_1, keys.at[aligned(slot * block, block)], r.kb_sem.at[slot])

    def fetch_v(p, b):
        slot = lax.rem(b, 2)
        fetch(p, b, r.v_own, r.v_all, r.v_all_1, values.at[aligned(slot * block, block)], r.vb_sem.at[slot])

    def have_k(b):
        slot = lax.rem(b, 3)
        pltpu.make_async_copy(r.k_all_1.at[0], keys.at[aligned(slot * block, block)], r.kb_sem.at[slot]).wait()

    def have_v(b):
        slot = lax.rem(b, 2)
        pltpu.make_async_copy(r.v_all_1.at[0], values.at[aligned(slot * block, block)], r.vb_sem.at[slot]).wait()

    def begin_pass(p):
        fetch_k(p, 0)
        fetch_v(p, 0)

        @pl.when(pass_size(p) > 1)
        def _():
            fetch_k(p, 1)

    def raw_scores(c, head, slot):
        query = jnp.concatenate([qo[chunk_rows(c), (head * groups + g) * HEAD:(head * groups + g + 1) * HEAD] for g in range(groups)], axis=0)
        scores_refs[head][...] = dot_t(query, keys[aligned(slot * block, block), head * HEAD:(head + 1) * HEAD])

    def state(c, head, low, length):
        return aligned(lax.rem(c, 2) * half + head * stack + low, length)

    def absorb(c, head, slot, bound):
        value = values[aligned(slot * block, block), head * HEAD:(head + 1) * HEAD]
        for low in range(0, stack, step):
            scores = scores_refs[head][low:low + step, :]
            if bound is not None:
                limit, by_row = bound
                row_id = lax.rem(low, chunk) + lax.rem(lax.broadcasted_iota(jnp.int32, scores.shape, 0), chunk)
                scores = jnp.where(lax.broadcasted_iota(jnp.int32, scores.shape, 1) < limit + by_row * row_id, scores, NEG_BIG)
            these = state(c, head, low, step)
            old = top[these, :]
            new = jnp.maximum(old, jnp.max(scores, axis=-1, keepdims=True))
            decay = jnp.exp(old - new)
            prob = jnp.exp(scores - jnp.concatenate([new] * (block // 128), axis=1))
            lanes = prob[:, :128]
            for i in range(1, block // 128):
                lanes = lanes + prob[:, i * 128:(i + 1) * 128]
            sums[these, :] = sums[these, :] * decay + lanes
            top[these, :] = new
            acc_ref[these, :] = acc_ref[these, :] * jnp.concatenate([decay] * (HEAD // 128), axis=1) + dot(prob.astype(BF16), value)

    def job_step(j, carry):
        second = j // 6
        c = (1 - second) * lax.rem(j, 2) + second * (j // 3)
        p = (1 - second) * (j // 2) + second * lax.rem(j, 3)

        @pl.when((j < 2) | (j == 3))
        def _():
            low = j - j // 3

            def body(i, carry):
                global_project(i)
                after = lead + 16 + 4 * i + 2 * (i // 2)
                event_loop(after, after + 1 + i // 2 - 2 * (i // 3))
                return carry
            lax.fori_loop(low, low + 1 + j // 3, body, 0)

            @pl.when(j == 3)
            def _():
                start_wo(1)

        @pl.when(p == 0)
        def _():
            for ref, value in ((top, NEG_BIG), (sums, 0.0), (acc_ref, 0.0)):
                ref[state(c, 0, 0, half), :] = jnp.full((half, ref.shape[1]), value, F32)
        count = pass_size(p)
        n_free = jnp.where(p == 2, cp, n_pass - n_mask)
        third = lax.rem(j, 3)
        base = jnp.where(second == 1, n_tick + jnp.where(j < 9, 3 * third, 6 + 2 * third), lead + 17 + 4 * j - 2 * (j // 2))
        begins = jnp.where((j == 1) | (j == 7) | (j == 9), 4, 1)
        eventful = (p < 2) & (j != 3)
        have_k(0)
        raw_scores(c, 0, 0)

        def block_step(masked, b, carry):
            have_v(b)

            @pl.when(b + 1 < count)
            def _():
                have_k(b + 1)
                fetch_v(p, b + 1)

            @pl.when(b + 2 < count)
            def _():
                fetch_k(p, b + 2)
            bound = None
            if masked:
                limit = jnp.where(p == 2, row_start(c) + 1, jnp.where(shard_of(p, b) == size - 1, first_pos - (size - 1) * shard - lax.rem(b, per_shard) * block, block))
                bound = (limit, jnp.where(p == 2, 1, 0))
            slot, later, v_slot = lax.rem(b, 3), lax.rem(b + 1, 3), lax.rem(b, 2)
            raw_scores(c, 1, slot)
            absorb(c, 0, v_slot, bound)
            raw_scores(c, 0, later)
            absorb(c, 1, v_slot, bound)

            @pl.when(eventful & (b >= begins) & (lax.rem(b - begins, 5) == 0))
            def _():
                event(base + (b - begins) // 5)
            return carry
        lax.fori_loop(0, n_free, functools.partial(block_step, False), 0)
        lax.fori_loop(n_free, count, functools.partial(block_step, True), 0)

        @pl.when(j == 1)
        def _():
            def body(i, carry):
                for copy in c_relay(i):
                    copy.wait_recv()
                return carry
            lax.fori_loop(0, per_shard, body, 0)

        @pl.when(j == 3)
        def _():
            free_fresh(2)
            free_fresh(3)

            def body(i, carry):
                for copy in new_sends(i):
                    copy.wait_recv()
                return carry
            lax.fori_loop(0, N_CHUNK, body, 0)

        @pl.when(j < 11)
        def _():
            after = j + 1
            begin_pass((1 - after // 6) * (after // 2) + (after // 6) * lax.rem(after, 3))

        @pl.when(p == 2)
        def _():
            these = chunk_rows(c)
            for head in range(n_kv):
                whole = state(c, head, 0, stack)
                total = jnp.sum(sums[whole, :], axis=-1, keepdims=True)
                result = (acc_ref[whole, :] / total).astype(BF16)
                for g in range(groups):
                    qo[these, (head * groups + g) * HEAD:(head * groups + g + 1) * HEAD] = result[g * chunk:(g + 1) * chunk]
            project_chunk(1, c)

        @pl.when((j == 8) | (j == 11))
        def _():
            event(jnp.where(j == 8, n_tick + 5, n_tick + 11))
        return carry
    for copy in c_near:
        copy.wait()
    begin_pass(jnp.int32(0))
    lax.fori_loop(0, 12, job_step, 0)
    start_gu(1)
    clock = n_tick + 12
    feed_forward(1, clock)
    event_loop(clock + N_CHUNK * N_SUB, 2 * n_tick)

    def finish(m, carry):
        out_copy(m).wait()
        return carry
    lax.fori_loop(0, per, finish, 0)

    def gathered(i, carry):
        for copy in c_across(i) + c_relay(i):
            copy.wait_send()
        return carry
    lax.fori_loop(0, per_shard, gathered, 0)


def run_layers(ins, collective_id):
    rows, dim = ins['x'].shape
    q_cols, kv_cols, ff = ins['w_query'].shape[2], ins['w_key'].shape[2], ins['w_gate'].shape[2]
    shard = ins['k_own'].shape[0]
    chunk = rows // N_CHUNK
    sub = chunk // N_SUB
    n_ev = 2 * N_CHUNK * N_SUB
    groups, n_kv = q_cols // kv_cols, kv_cols // HEAD
    stack = groups * chunk
    pieces = 2 * (shard // rows)

    def spec(name):
        if name == 'first_pos':
            return pl.BlockSpec(memory_space=pltpu.SMEM)
        return pl.BlockSpec(memory_space=pltpu.VMEM if name in ('gains', 'qk_gains') else pl.ANY)
    array = jax.ShapeDtypeStruct
    made = array((rows, kv_cols), BF16)
    outs = dict(x_out=array((rows, dim), BF16), k_new_0=made, v_new_0=made, k_new_1=made, v_new_1=made)
    outs |= dict(k_all=array((4, shard, kv_cols), BF16), v_all=array((4, shard, kv_cols), BF16), k_all_1=array((4, rows, kv_cols), BF16), v_all_1=array((4, rows, kv_cols), BF16))
    dma = pltpu.SemaphoreType.DMA
    scratch = dict(
        part=pltpu.VMEM((rows, dim), BF16),
        tot=pltpu.VMEM((rows, dim), BF16),
        xv=pltpu.VMEM((rows, dim), BF16),
        wt=pltpu.VMEM((W_SLOTS, dim, TILE), BF16),
        dn=pltpu.VMEM((D_SLOTS, ff, TILE), BF16),
        qo=pltpu.VMEM((rows, q_cols), BF16),
        hact=pltpu.VMEM((chunk, ff), BF16),
        recv2=pltpu.VMEM((RECV_SLOTS, sub, dim), BF16),
        keys=pltpu.VMEM((3 * rows, kv_cols), BF16),
        values=pltpu.VMEM((2 * rows, kv_cols), BF16),
        fresh=pltpu.VMEM((2, 2, chunk, kv_cols), BF16),
        turn=pltpu.VMEM((2, chunk, HEAD // 2), F32),
        s_even=pltpu.VMEM((stack, rows), F32),
        s_odd=pltpu.VMEM((stack, rows), F32),
        top=pltpu.VMEM((2 * n_kv * stack, 128), F32),
        sums=pltpu.VMEM((2 * n_kv * stack, 128), F32),
        acc=pltpu.VMEM((2 * n_kv * stack, HEAD), F32),
        w_sem=dma((W_SLOTS,)), wo_sem=dma((W_SLOTS * (dim // q_cols),)), dn_sem=dma((D_SLOTS,)), x_sem=dma((N_CHUNK,)), t_sem=dma((2,)), old_sem=dma((2,)),
        kv_sem=dma((2,)), own_sem=dma((2, 4)), kb_sem=dma((3,)), vb_sem=dma((2,)), out_sem=dma((n_ev // 2,)),
        w_s=dma((2 * N_CHUNK,)), w_r=dma((2 * N_CHUNK,)), n_s=dma((6 * N_CHUNK,)), n_r=dma((6 * N_CHUNK,)),
        c_near_s=dma((2,)), c_near_r=dma((2,)), c_across_s=dma((pieces,)), c_across_r=dma((pieces,)), c_relay_s=dma((pieces,)), c_relay_r=dma((pieces,)),
        s1=dma((n_ev,)), s2s=dma((n_ev,)), s2r=dma((n_ev,)), s3=dma((n_ev,)),
        credit=pltpu.SemaphoreType.REGULAR,
    )
    names = tuple(ins) + tuple(outs) + tuple(scratch)
    made = pl.pallas_call(
        functools.partial(layers_kernel, names),
        out_shape=tuple(outs.values()),
        in_specs=[spec(name) for name in ins],
        out_specs=tuple(pl.BlockSpec(memory_space=pl.ANY) for _ in outs),
        scratch_shapes=list(scratch.values()),
        compiler_params=pltpu.CompilerParams(collective_id=collective_id, has_side_effects=True, vmem_limit_bytes=VMEM_LIMIT),
        name='two_layers',
    )(*ins.values())
    return dict(zip(outs, made))


def leave_kernel(n_kv, *refs):
    half = len(refs) // 2
    refs[half][...] = refs[0][...]
    for flat, shaped in zip(refs[1:half], refs[half + 1:]):
        for head in range(n_kv):
            shaped[:, head, :] = flat[:, head * HEAD:(head + 1) * HEAD]


def leave(x, *flats):
    rows, dim = x.shape
    kv_cols = flats[0].shape[1]
    n_kv, step = kv_cols // HEAD, rows // 8
    wide = pl.BlockSpec((step, dim), lambda i: (i, 0))
    flat = pl.BlockSpec((step, kv_cols), lambda i: (i, 0))
    shaped = pl.BlockSpec((step, n_kv, HEAD), lambda i: (i, 0, 0))
    return pl.pallas_call(
        functools.partial(leave_kernel, n_kv),
        grid=(8,),
        out_shape=(jax.ShapeDtypeStruct((rows, dim), BF16),) + (jax.ShapeDtypeStruct((rows, n_kv, HEAD), BF16),) * len(flats),
        in_specs=[wide] + [flat] * len(flats),
        out_specs=(wide,) + (shaped,) * len(flats),
        name='leave',
    )(x, *flats)


def solution(mesh):
    row_spec = P(('dp', 'cp'), None)
    cache_spec = P(('dp', 'cp'), 'tp', None)
    window_spec = P('dp', 'tp', None)
    col_spec = P(None, None, 'tp')
    row_split = P(None, 'tp', None)
    replicated = P()

    def device_step(hidden, start_pos, k_local, v_local, k_global, v_global, w_query, w_key, w_value, w_out, w_gate, w_up, w_down, norm_gain, qk_gain):
        first_pos = start_pos[0]
        cp_index = lax.axis_index('cp')
        rows, dim = hidden.shape
        window = k_local.shape[0]
        flat = lambda a: a.reshape(a.shape[0], -1)
        gains = jnp.concatenate([norm_gain.reshape(8, dim), jnp.zeros((8, dim), F32)], axis=0)
        qk_gains = jnp.concatenate([qk_gain.reshape(4, HEAD), jnp.zeros((4, HEAD), F32)], axis=0)
        turn = jnp.remainder(first_pos, window)
        rolled = [flat(lax.dynamic_slice_in_dim(jnp.concatenate([a, a], axis=0), turn, window, axis=0)) for a in (k_local, v_local)]
        cos_local, sin_local = rope_tables(first_pos + cp_index * rows, rows, LOCAL_BASE, 1.0)
        cos_global, sin_global = rope_tables(first_pos + cp_index * rows, rows, GLOBAL_BASE, GLOBAL_DIV)
        made = run_layers(dict(
            first_pos=start_pos, x=hidden, gains=gains, qk_gains=qk_gains,
            cos_local=cos_local, sin_local=sin_local, cos_global=cos_global, sin_global=sin_global,
            w_query=w_query, w_key=w_key, w_value=w_value, w_out=w_out, w_gate=w_gate, w_up=w_up, w_down=w_down,
            k_old=rolled[0], v_old=rolled[1], k_own=flat(k_global), v_own=flat(v_global),
        ), 0)
        return leave(made['x_out'], made['k_new_0'], made['v_new_0'], made['k_new_1'], made['v_new_1'])

    return jax.shard_map(device_step, mesh=mesh, in_specs=(row_spec, P('dp'), window_spec, window_spec, cache_spec, cache_spec, col_spec, col_spec, col_spec, row_split, col_spec, col_spec, row_split, replicated, replicated), out_specs=(row_spec, cache_spec, cache_spec, cache_spec, cache_spec), check_vma=False)
```
